32 devices in a mesh: grp: 2 (over core), row: 4 (over y, x), col: 4 (over z).
Axes of the slice: x: 2, y: 2, z: 4, core: 2. Of those that a mesh axis runs over, the one named last changes fastest.
Arguments:
- sub_rhs: float32 [2, 3, 4, 4, 256, 512], P('grp', None, 'row', 'col'), may hold values from -6 to 6
- sub_dinv: float32 [2, 3, 4, 4, 256, 256], P('grp', None, 'row', 'col')
- anc_rhs: float32 [4, 4, 256, 512], P('row', 'col'), may hold values from -6 to 6
- anc_dinv: float32 [4, 4, 256, 256], P('row', 'col')
- tiles: bfloat16 [2, 4, 4, 3, 16, 256, 256], P('grp', 'row', 'col'), may hold values from -0.09375 to 0.09375
- tile_target: int32 [2, 4, 4, 3, 16], P('grp', 'row', 'col'), may hold values from 0 to 11, as said below
- tile_source: int32 [2, 4, 4, 3, 16], P('grp', 'row', 'col'), may hold values from 0 to 3, as said below
- tile_count: int32 [2, 4, 4, 3], P('grp', 'row', 'col'), may hold values from 1 to 16, as said below
Outputs:
- sub_solution: float32 [2, 3, 4, 4, 256, 512], P('grp', None, 'row', 'col')
- anc_solution: float32 [4, 4, 256, 512], P('row', 'col')
The draws below stay inside these ranges and needn't reach their ends.
Inputs may be any that keep to these rules, and one draw needn't show every extreme that they name: `tile_target`: entry [g, q, c, k, j] is (t - 1) * 4 + r for a target level t with k < t <= 3 (t = 3 is the ancestor level) and a process row r; entries at slots j >= tile_count are unused. `tile_source`: Non-decreasing along the last dimension. `tile_count`: for every source level some device holds exactly 16 live tiles.
All inputs are finite; a program needn't handle non-finite values.
Results may differ from the reference program's by a relative error of at most 0.0027.
Values may be sent and summed in bfloat16 or wider, within the bound.
A program may use at most 128 MiB of HBM per device.

```python
import math
import jax
import jax.numpy as jnp
from jax import lax

S = 256
LEV = 3
TPS = 16
W = 512
N_GRP = 2
N_ROW = 4
N_COL = 4


def inverse_blocks(key, shape):
    noise = jax.random.normal(key, shape, jnp.float32)
    return jnp.eye(S, dtype=jnp.float32) + 0.5 * noise / math.sqrt(S)


def draw_sub_dinv(key, part):
    return inverse_blocks(jax.random.fold_in(key, 11), (N_GRP, LEV, N_ROW, N_COL, S, S))


def draw_anc_dinv(key, part):
    return inverse_blocks(jax.random.fold_in(key, 13), (N_ROW, N_COL, S, S))


def draw_tile_target(key, part):
    shape = (N_GRP, N_ROW, N_COL, LEV, TPS)
    first_key, second_key = jax.random.split(jax.random.fold_in(key, 17))
    level_ids = lax.broadcasted_iota(jnp.int32, shape, 3)
    steps_up = jax.random.randint(first_key, shape, 0, 1048576) % (LEV - level_ids)
    target_rows = jax.random.randint(second_key, shape, 0, N_ROW)
    return ((level_ids + steps_up) * N_ROW + target_rows).astype(jnp.int32)


def draw_tile_source(key, part):
    shape = (N_GRP, N_ROW, N_COL, LEV, TPS)
    picked = jax.random.randint(jax.random.fold_in(key, 19), shape, 0, N_COL)
    return jnp.sort(picked, axis=-1).astype(jnp.int32)


def draw_tile_count(key, part):
    places = N_GRP * N_ROW * N_COL
    first_key, second_key = jax.random.split(jax.random.fold_in(key, 23))
    shifts = jax.random.randint(first_key, (places, LEV), 0, 4)
    base = jnp.maximum(TPS // jnp.left_shift(jnp.ones_like(shifts), shifts), 1)
    chosen = jax.random.randint(second_key, (LEV,), 0, places)
    place_ids = lax.broadcasted_iota(jnp.int32, (places, LEV), 0)
    counts = jnp.where(place_ids == chosen[None, :], TPS, base)
    return counts.reshape(N_GRP, N_ROW, N_COL, LEV).astype(jnp.int32)


def steps_of(key, dims, pieces, least, largest):
    factor_of = 1.0
    for axis_at, blocks in pieces:
        heights = jax.random.uniform(jax.random.fold_in(jax.random.fold_in(key, 6), axis_at), (blocks,), jnp.float32, least / len(pieces), largest / len(pieces))
        factor_of = factor_of * jnp.repeat(jnp.exp(heights), dims[axis_at] // blocks).reshape((-1,) + (1,) * (len(dims) - 1 - axis_at))
    return factor_of


def normal_values(key, shape, deviation, bound, cuts=(), kind=jnp.bfloat16):
    array = deviation * jax.random.normal(key, shape, jnp.float32)
    if cuts:
        array = array * steps_of(key, shape, cuts, -0.22, 0.18)
    return jnp.clip(array, -bound, bound).astype(kind)


def setup_inputs(seed: int = 0) -> dict:
    splits = jax.random.split(jax.random.key(seed), 9)
    return {
        "sub_rhs": normal_values(splits[0], (N_GRP, LEV, N_ROW, N_COL, S, W), 1.0, 6.0, ((0, 2), (2, 4), (3, 4)), jnp.float32),
        "sub_dinv": draw_sub_dinv(jax.random.fold_in(splits[8], 71), 0),
        "anc_rhs": normal_values(splits[2], (N_ROW, N_COL, S, W), 1.0, 6.0, ((0, 4), (1, 4)), jnp.float32),
        "anc_dinv": draw_anc_dinv(jax.random.fold_in(splits[8], 71), 0),
        "tiles": normal_values(splits[4], (N_GRP, N_ROW, N_COL, LEV, TPS, S, S), (S * TPS) ** -0.5, 0.09375, ((0, 2), (1, 4), (2, 4))),
        "tile_target": draw_tile_target(jax.random.fold_in(splits[8], 71), 0),
        "tile_source": draw_tile_source(jax.random.fold_in(splits[8], 71), 0),
        "tile_count": draw_tile_count(jax.random.fold_in(splits[8], 71), 0),
    }


def reference(sub_rhs, sub_dinv, anc_rhs, anc_dinv, tiles, tile_target, tile_source, tile_count):
    highest = lax.Precision.HIGHEST
    slot_ids = jnp.arange(TPS, dtype=jnp.int32)
    column_ids = jnp.broadcast_to(jnp.arange(N_COL, dtype=jnp.int32)[:, None], (N_COL, TPS))
    ancestor_sum = jnp.zeros((N_ROW, N_COL, S, W), jnp.float32)
    groups_out = []
    for group in range(N_GRP):
        pending = jnp.zeros((LEV * N_ROW, N_COL, S, W), jnp.float32)
        solved = []
        for source_level in range(LEV):
            remainder = sub_rhs[group, source_level]
            if source_level > 0:
                remainder = remainder - pending[(source_level - 1) * N_ROW:source_level * N_ROW]
            current = jnp.einsum("rcij,rcjw->rciw", sub_dinv[group, source_level], remainder, precision=highest)
            solved.append(current)
            rounded = current.astype(jnp.bfloat16)
            for proc_row in range(N_ROW):
                sources = tile_source[group, proc_row, :, source_level]
                targets = tile_target[group, proc_row, :, source_level]
                live = slot_ids[None, :] < tile_count[group, proc_row, :, source_level][:, None]
                fetched = rounded[proc_row][sources].astype(jnp.float32)
                blocks = tiles[group, proc_row, :, source_level].astype(jnp.float32)
                products = jnp.einsum("ctij,ctjw->ctiw", blocks, fetched, precision=highest)
                products = jnp.where(live[:, :, None, None], products, jnp.zeros_like(products))
                pending = pending.at[targets, column_ids].add(products)
        ancestor_sum = ancestor_sum + pending[(LEV - 1) * N_ROW:]
        groups_out.append(jnp.stack(solved))
    ancestor = jnp.einsum("rcij,rcjw->rciw", anc_dinv, anc_rhs - ancestor_sum, precision=highest)
    return jnp.stack(groups_out), ancestor
```

```python
import functools

import jax
import jax.numpy as jnp
from jax import lax
from jax.experimental import pallas as pl
from jax.experimental.pallas import tpu as pltpu
from jax.sharding import PartitionSpec as P

MESH = pl.DeviceIdType.MESH
CHUNK = 128
AHEAD = 3
LAG = 1


def hops(n_col):
    if not 2 < n_col <= 4:
        return ()
    up = [(o, n_col - 2, n_col - 1) for o in reversed(range(n_col - 2))]
    down = [(o, 1, 0) for o in range(2, n_col)]
    return tuple(up + down)


def kernel(
    n_grp, n_row, n_col,
    target_hbm, source_hbm, count_hbm,
    rhs_hbm, inv_hbm, anc_rhs_hbm, anc_inv_hbm, tiles_hbm,
    sub_out, anc_out,
    rhs, inv, anc_rhs, anc_inv, tiles,
    gathered, fetched, chain, pending, outbox, inbox, anc_box,
    target_ref, source_ref, count_ref, prev_s, last_s, src_s,
    load_sem, ag_send, ag_recv, fwd_send, rs_send, rs_recv, anc_send, anc_recv,
):
    depth, size, width = rhs.shape
    slots = tiles.shape[1]
    chunks = width // CHUNK
    steps = depth * chunks
    codes = depth * n_row
    passes = hops(n_col)
    g = lax.axis_index("grp")
    q = lax.axis_index("row")
    c = lax.axis_index("col")

    early = [
        pltpu.make_async_copy(inv_hbm.at[0], inv.at[0], load_sem.at[0]),
        pltpu.make_async_copy(rhs_hbm.at[0], rhs.at[0], load_sem.at[1]),
    ]
    maps = [
        pltpu.make_async_copy(target_hbm, target_ref, load_sem.at[7]),
        pltpu.make_async_copy(source_hbm, source_ref, load_sem.at[8]),
        pltpu.make_async_copy(count_hbm, count_ref, load_sem.at[9]),
    ]
    loads = [
        pltpu.make_async_copy(tiles_hbm, tiles, load_sem.at[2]),
        pltpu.make_async_copy(anc_rhs_hbm, anc_rhs, load_sem.at[3]),
        pltpu.make_async_copy(anc_inv_hbm, anc_inv, load_sem.at[4]),
    ]
    if depth > 1:
        loads += [
            pltpu.make_async_copy(inv_hbm.at[pl.ds(1, depth - 1)], inv.at[pl.ds(1, depth - 1)], load_sem.at[5]),
            pltpu.make_async_copy(rhs_hbm.at[pl.ds(1, depth - 1)], rhs.at[pl.ds(1, depth - 1)], load_sem.at[6]),
        ]
    for load in early:
        load.start()

    barrier = pltpu.get_barrier_semaphore()
    apart = [(o, e) for o, _, e in passes if (e, o) in [(a, b) for a, _, b in passes]]
    strangers = sum((c == o).astype(jnp.int32) for o, _ in apart) if apart else 0
    for d in range(1, n_col):
        peer = lax.rem(c + d, n_col)
        met = True
        for o, e in apart:
            met = met & jnp.logical_not((c == o) & (peer == e))

        @pl.when(met)
        def _():
            pl.semaphore_signal(barrier, inc=1, device_id=(g, q, peer), device_id_type=MESH)

    for e in range(n_grp):
        for d in range(n_row):
            if e or d:
                pl.semaphore_signal(
                    barrier, inc=1,
                    device_id=(lax.rem(g + e, n_grp), lax.rem(q + d, n_row), c), device_id_type=MESH,
                )

    def tables(k, carry):
        count = count_ref[0, 0, 0, k]
        raw = [target_ref[k, 0, j] for j in range(slots)]
        live = [jnp.where(j < count, raw[j], -1) for j in range(slots)]
        for j in range(slots):
            found = jnp.int32(0)
            for i in range(j):
                found = jnp.where(raw[i] == raw[j], i + 1, found)
            prev_s[k * slots + j] = found
            src_s[k * slots + j] = jnp.clip(source_ref[k, 0, j], 0, n_col - 1)
        for code in range(codes):
            found = jnp.int32(0)
            for j in range(slots):
                found = jnp.where(live[j] == code, j + 1, found)
            last_s[k * codes + code] = found
        return carry

    def cols(w):
        return pl.ds(pl.multiple_of(w * CHUNK, CHUNK), CHUNK)

    def ag_copy(i, owner, peer):
        return pltpu.make_async_remote_copy(
            src_ref=gathered.at[i, owner], dst_ref=gathered.at[i, owner],
            send_sem=ag_send.at[i, peer], recv_sem=ag_recv.at[i, owner],
            device_id=(g, q, peer), device_id_type=MESH,
        )

    def relays(i, run):
        for way, (owner, relay, end) in enumerate(passes):

            @pl.when(c == relay)
            def _():
                run(
                    ag_copy(i, owner, c),
                    pltpu.make_async_remote_copy(
                        src_ref=gathered.at[i, owner], dst_ref=gathered.at[i, owner],
                        send_sem=fwd_send.at[i, way], recv_sem=ag_recv.at[i, owner],
                        device_id=(g, q, end), device_id_type=MESH,
                    ),
                )

    def each_direct(i, run):
        for d in range(1, n_col):
            peer = lax.rem(c + d, n_col)
            far = False
            for owner, relay, end in passes:
                far = far | ((c == owner) & (peer == end))

            @pl.when(jnp.logical_not(far))
            def _():
                run(ag_copy(i, c, peer), held(i, peer))

    def held(i, peer):
        if not passes:
            return False
        to_end = ((c == n_col - 2) & (peer == n_col - 1)) | ((c == 1) & (peer == 0))
        return to_end & (i >= AHEAD) & (i < chunks)

    def send_direct(i):
        def start(copy, wait_turn):
            pl.when(jnp.logical_not(wait_turn))(copy.start)

        each_direct(i, start)

    def release(i):
        for relay, end in ((n_col - 2, n_col - 1), (1, 0)):
            if passes:

                @pl.when((c == relay) & (i + AHEAD < chunks))
                def _():
                    ag_copy(i + AHEAD, c, end).start()

    def rs_copy(i, owner_g, owner_q, to_g, to_q):
        return pltpu.make_async_remote_copy(
            src_ref=outbox.at[i, to_q], dst_ref=inbox.at[i, owner_g * n_row + owner_q],
            send_sem=rs_send.at[i, to_q], recv_sem=rs_recv.at[i, owner_g * n_row + owner_q],
            device_id=(to_g, to_q, c), device_id_type=MESH,
        )

    def anc_copy(w, peer_g):
        return pltpu.make_async_remote_copy(
            src_ref=anc_box.at[w], dst_ref=anc_box.at[w],
            send_sem=anc_send.at[w, peer_g], recv_sem=anc_recv.at[w],
            device_id=(peer_g, q, c), device_id_type=MESH,
        )

    def full_dot(a, b):
        return jnp.dot(a, b, precision=lax.Precision.HIGHEST, preferred_element_type=jnp.float32)

    def solve(i, k, w, first):
        rest = rhs[k, :, cols(w)]
        if not first:
            back = i - chunks
            total = pending[w, (k - 1) * n_row + q]
            for d in range(1, n_row):
                other = lax.rem(q + d, n_row)
                rs_copy(back, g, other, g, q).wait_recv()
                total = total + inbox[back, g * n_row + other].astype(jnp.float32)
            rest = rest - total
        answer = full_dot(inv[k], rest)
        sub_out[k, :, cols(w)] = answer
        gathered[i, c] = answer.astype(jnp.bfloat16)

    def pass_on(arrived, onward):
        arrived.wait_recv()
        onward.start()

    def spread(i, k, w):
        relays(i, pass_on)
        release(i)
        for d in range(1, n_col):
            other = lax.rem(c + d, n_col)
            passed = False
            for owner, relay, end in passes:
                passed = passed | ((c == relay) & (other == owner))

            @pl.when(jnp.logical_not(passed))
            def _():
                ag_copy(i, other, c).wait_recv()

        for s in range(n_col):
            fetched[s] = gathered[i, s]

        for j in range(slots):
            product = jnp.dot(
                tiles[k, j], fetched[src_s[k * slots + j]], preferred_element_type=jnp.float32
            )
            chain[j + 1] = product + chain[prev_s[k * slots + j]]

        def updated(code):
            return pending[w, code] + chain[last_s[k * codes + code]]

        to_g = jnp.where(k < depth - 1, g, lax.rem(w, n_grp))
        for d in list(range(1, n_row)) + [0]:
            to_q = lax.rem(q + d, n_row)
            value = updated(k * n_row + to_q)

            def send():
                outbox[i, to_q] = value.astype(jnp.bfloat16)
                rs_copy(i, g, q, to_g, to_q).start()

            if d == 0:
                pending[w, k * n_row + q] = value
                pl.when(to_g != g)(send)
            else:
                send()

        def collect(code, carry):
            pending[w, code] = updated(code)
            return carry

        lax.fori_loop((k + 1) * n_row, codes, collect, 0)

    def finish(w):
        i = (depth - 1) * chunks + w

        @pl.when(lax.rem(w, n_grp) == g)
        def _():
            total = pending[w, (depth - 1) * n_row + q]
            for e in range(n_grp):
                for d in range(n_row):
                    if e or d:
                        other_g, other_q = lax.rem(g + e, n_grp), lax.rem(q + d, n_row)
                        rs_copy(i, other_g, other_q, g, q).wait_recv()
                        total = total + inbox[i, other_g * n_row + other_q].astype(jnp.float32)
            anc_box[w] = full_dot(anc_inv[...], anc_rhs[:, cols(w)] - total)
            for e in range(1, n_grp):
                anc_copy(w, lax.rem(g + e, n_grp)).start()

    for load in early:
        load.wait()
    for load in maps + loads:
        load.start()
    solve(0, 0, 0, True)
    pl.semaphore_wait(barrier, n_col - 1 + n_grp * n_row - 1 - strangers)

    send_direct(0)

    def first_level(w, carry):
        solve(w, 0, w, True)
        send_direct(w)
        return carry

    lax.fori_loop(1, chunks, first_level, 0)
    for load in maps:
        load.wait()
    lax.fori_loop(0, depth, tables, 0)
    chain[0] = jnp.zeros(chain.shape[1:], jnp.float32)

    def clear(n, carry):
        pending[n // codes, lax.rem(n, codes)] = jnp.zeros(pending.shape[2:], jnp.float32)
        return carry

    lax.fori_loop(0, chunks * codes, clear, 0)
    for load in loads:
        load.wait()

    def middle(i, carry):
        spread(i, i // chunks, lax.rem(i, chunks))
        later = i + chunks - LAG

        @pl.when((i >= LAG) & (later < steps))
        def _():
            solve(later, later // chunks, lax.rem(later, chunks), False)
            send_direct(later)

        @pl.when(later >= steps)
        def _():
            finish(later - steps)

        return carry

    lax.fori_loop(0, steps, middle, 0)
    for w in range(chunks - LAG, chunks):
        finish(jnp.int32(w))

    def deliver(w, carry):
        owner = lax.rem(w, n_grp)

        @pl.when(owner != g)
        def _():
            anc_copy(w, g).wait_recv()

        anc_out[:, cols(w)] = anc_box[w]

        @pl.when(owner == g)
        def _():
            for e in range(1, n_grp):
                anc_copy(w, lax.rem(g + e, n_grp)).wait_send()

        return carry

    lax.fori_loop(0, chunks, deliver, 0)

    def drain(i, carry):
        each_direct(i, lambda copy, wait_turn: copy.wait_send())
        relays(i, lambda arrived, onward: onward.wait_send())
        to_g = jnp.where(i < (depth - 1) * chunks, g, lax.rem(lax.rem(i, chunks), n_grp))
        for d in range(1, n_row):
            rs_copy(i, g, q, to_g, lax.rem(q + d, n_row)).wait_send()

        @pl.when(to_g != g)
        def _():
            rs_copy(i, g, q, to_g, q).wait_send()

        return carry

    lax.fori_loop(0, steps, drain, 0)


def hand_over(sub_ref, anc_ref, sub_out, anc_out, sem):
    copies = [
        pltpu.make_async_copy(sub_ref, sub_out, sem.at[0]),
        pltpu.make_async_copy(anc_ref, anc_out, sem.at[1]),
    ]
    for copy in copies:
        copy.start()
    for copy in copies:
        copy.wait()


def on_device(mesh, sub_rhs, sub_dinv, anc_rhs, anc_dinv, tiles, tile_target, tile_source, tile_count):
    n_grp, n_row, n_col = mesh.shape["grp"], mesh.shape["row"], mesh.shape["col"]
    depth, size, width = sub_rhs.shape[1], sub_rhs.shape[4], sub_rhs.shape[5]
    slots = tiles.shape[4]
    chunks = width // CHUNK
    steps = depth * chunks
    codes = depth * n_row
    bf16, f32 = jnp.bfloat16, jnp.float32
    dma = pltpu.SemaphoreType.DMA
    sub, anc = pl.pallas_call(
        functools.partial(kernel, n_grp, n_row, n_col),
        out_shape=(
            pltpu.VMEM((depth, size, width), f32),
            pltpu.VMEM((size, width), f32),
        ),
        in_specs=[pl.BlockSpec(memory_space=pltpu.HBM)] * 8,
        out_specs=(pl.BlockSpec(memory_space=pltpu.VMEM), pl.BlockSpec(memory_space=pltpu.VMEM)),
        scratch_shapes=[
            pltpu.VMEM((depth, size, width), f32),
            pltpu.VMEM((depth, size, size), f32),
            pltpu.VMEM((size, width), f32),
            pltpu.VMEM((size, size), f32),
            pltpu.VMEM((depth, slots, size, size), bf16),
            pltpu.VMEM((steps, n_col, size, CHUNK), bf16),
            pltpu.VMEM((n_col, size, CHUNK), bf16),
            pltpu.VMEM((slots + 1, size, CHUNK), f32),
            pltpu.VMEM((chunks, codes, size, CHUNK), f32),
            pltpu.VMEM((steps, n_row, size, CHUNK), bf16),
            pltpu.VMEM((steps, n_grp * n_row, size, CHUNK), bf16),
            pltpu.VMEM((chunks, size, CHUNK), f32),
            pltpu.SMEM((depth, 1, slots), jnp.int32),
            pltpu.SMEM((depth, 1, slots), jnp.int32),
            pltpu.SMEM((1, 1, 1, depth), jnp.int32),
            pltpu.SMEM((depth * slots,), jnp.int32),
            pltpu.SMEM((depth * codes,), jnp.int32),
            pltpu.SMEM((depth * slots,), jnp.int32),
            dma((10,)),
            dma((steps, n_col)),
            dma((steps, n_col)),
            dma((steps, max(len(hops(n_col)), 1))),
            dma((steps, n_row)),
            dma((steps, n_grp * n_row)),
            dma((chunks, n_grp)),
            dma((chunks,)),
        ],
        compiler_params=pltpu.CompilerParams(
            collective_id=0, has_side_effects=True, vmem_limit_bytes=67_043_328 - 4 * (depth + 1) * size * width
        ),
    )(
        tile_target.reshape(depth, 1, slots), tile_source.reshape(depth, 1, slots), tile_count,
        sub_rhs.reshape(depth, size, width), sub_dinv.reshape(depth, size, size),
        anc_rhs.reshape(size, width), anc_dinv.reshape(size, size),
        tiles.reshape(depth, slots, size, size),
    )
    sub, anc = pl.pallas_call(
        hand_over,
        out_shape=(
            jax.ShapeDtypeStruct((depth, size, width), f32),
            jax.ShapeDtypeStruct((size, width), f32),
        ),
        in_specs=[pl.BlockSpec(memory_space=pl.ANY)] * 2,
        out_specs=(pl.BlockSpec(memory_space=pl.ANY), pl.BlockSpec(memory_space=pl.ANY)),
        scratch_shapes=[dma((2,))],
        compiler_params=pltpu.CompilerParams(vmem_limit_bytes=1 << 20),
    )(sub, anc)
    return sub[None, :, None, None], anc[None, None]


def solution(mesh):
    placed = (
        P("grp", None, "row", "col", None, None),
        P("grp", None, "row", "col", None, None),
        P("row", "col", None, None),
        P("row", "col", None, None),
        P("grp", "row", "col", None, None, None, None),
        P("grp", "row", "col", None, None),
        P("grp", "row", "col", None, None),
        P("grp", "row", "col", None),
    )
    return jax.shard_map(
        functools.partial(on_device, mesh),
        mesh=mesh,
        in_specs=placed,
        out_specs=(P("grp", None, "row", "col", None, None), P("row", "col", None, None)),
        check_vma=False,
    )
```

```python
import functools

import jax
import jax.numpy as jnp
from jax import lax
from jax.experimental import pallas as pl
from jax.experimental.pallas import tpu as pltpu
from jax.sharding import PartitionSpec as P

MESH = pl.DeviceIdType.MESH
CHUNK = 128
AHEAD = 3
LAG = 1


def hops(n_col):
    if not 2 < n_col <= 4:
        return ()
    up = [(o, n_col - 2, n_col - 1) for o in reversed(range(n_col - 2))]
    down = [(o, 1, 0) for o in range(2, n_col)]
    return tuple(up + down)


def kernel(
    n_grp, n_row, n_col,
    target_hbm, source_hbm, count_hbm,
    rhs_hbm, inv_hbm, anc_rhs_hbm, anc_inv_hbm, tiles_hbm,
    sub_out, anc_out,
    rhs, inv, anc_rhs, anc_inv, tiles,
    gathered, fetched, chain, pending, outbox, inbox, anc_box,
    target_ref, source_ref, count_ref, prev_s, last_s, src_s,
    load_sem, ag_send, ag_recv, fwd_send, rs_send, rs_recv, anc_send, anc_recv,
):
    depth, size, width = rhs.shape
    slots = tiles.shape[1]
    chunks = width // CHUNK
    steps = depth * chunks
    codes = depth * n_row
    passes = hops(n_col)
    g = lax.axis_index("grp")
    q = lax.axis_index("row")
    c = lax.axis_index("col")

    early = [
        pltpu.make_async_copy(inv_hbm.at[0], inv.at[0], load_sem.at[0]),
        pltpu.make_async_copy(rhs_hbm.at[0], rhs.at[0], load_sem.at[1]),
    ]
    maps = [
        pltpu.make_async_copy(target_hbm, target_ref, load_sem.at[7]),
        pltpu.make_async_copy(source_hbm, source_ref, load_sem.at[8]),
        pltpu.make_async_copy(count_hbm, count_ref, load_sem.at[9]),
    ]
    loads = [
        pltpu.make_async_copy(tiles_hbm, tiles, load_sem.at[2]),
        pltpu.make_async_copy(anc_rhs_hbm, anc_rhs, load_sem.at[3]),
        pltpu.make_async_copy(anc_inv_hbm, anc_inv, load_sem.at[4]),
    ]
    if depth > 1:
        loads += [
            pltpu.make_async_copy(inv_hbm.at[pl.ds(1, depth - 1)], inv.at[pl.ds(1, depth - 1)], load_sem.at[5]),
            pltpu.make_async_copy(rhs_hbm.at[pl.ds(1, depth - 1)], rhs.at[pl.ds(1, depth - 1)], load_sem.at[6]),
        ]
    for load in early:
        load.start()

    barrier = pltpu.get_barrier_semaphore()
    apart = [(o, e) for o, _, e in passes if (e, o) in [(a, b) for a, _, b in passes]]
    strangers = sum((c == o).astype(jnp.int32) for o, _ in apart) if apart else 0
    for d in range(1, n_col):
        peer = lax.rem(c + d, n_col)
        met = True
        for o, e in apart:
            met = met & jnp.logical_not((c == o) & (peer == e))

        @pl.when(met)
        def _():
            pl.semaphore_signal(barrier, inc=1, device_id=(g, q, peer), device_id_type=MESH)

    for e in range(n_grp):
        for d in range(n_row):
            if e or d:
                pl.semaphore_signal(
                    barrier, inc=1,
                    device_id=(lax.rem(g + e, n_grp), lax.rem(q + d, n_row), c), device_id_type=MESH,
                )

    def tables(k, carry):
        count = count_ref[0, 0, 0, k]
        raw = [target_ref[k, 0, j] for j in range(slots)]
        live = [jnp.where(j < count, raw[j], -1) for j in range(slots)]
        for j in range(slots):
            found = jnp.int32(0)
            for i in range(j):
                found = jnp.where(raw[i] == raw[j], i + 1, found)
            prev_s[k * slots + j] = found
            src_s[k * slots + j] = jnp.clip(source_ref[k, 0, j], 0, n_col - 1)
        for code in range(codes):
            found = jnp.int32(0)
            for j in range(slots):
                found = jnp.where(live[j] == code, j + 1, found)
            last_s[k * codes + code] = found
        return carry

    def cols(w):
        return pl.ds(pl.multiple_of(w * CHUNK, CHUNK), CHUNK)

    def ag_copy(i, owner, peer):
        return pltpu.make_async_remote_copy(
            src_ref=gathered.at[i, owner], dst_ref=gathered.at[i, owner],
            send_sem=ag_send.at[i, peer], recv_sem=ag_recv.at[i, owner],
            device_id=(g, q, peer), device_id_type=MESH,
        )

    def relays(i, run):
        for way, (owner, relay, end) in enumerate(passes):

            @pl.when(c == relay)
            def _():
                run(
                    ag_copy(i, owner, c),
                    pltpu.make_async_remote_copy(
                        src_ref=gathered.at[i, owner], dst_ref=gathered.at[i, owner],
                        send_sem=fwd_send.at[i, way], recv_sem=ag_recv.at[i, owner],
                        device_id=(g, q, end), device_id_type=MESH,
                    ),
                )

    def each_direct(i, run):
        for d in range(1, n_col):
            peer = lax.rem(c + d, n_col)
            far = False
            for owner, relay, end in passes:
                far = far | ((c == owner) & (peer == end))

            @pl.when(jnp.logical_not(far))
            def _():
                run(ag_copy(i, c, peer), held(i, peer))

    def held(i, peer):
        if not passes:
            return False
        to_end = ((c == n_col - 2) & (peer == n_col - 1)) | ((c == 1) & (peer == 0))
        return to_end & (i >= AHEAD) & (i < chunks)

    def send_direct(i):
        def start(copy, wait_turn):
            pl.when(jnp.logical_not(wait_turn))(copy.start)

        each_direct(i, start)

    def release(i):
        for relay, end in ((n_col - 2, n_col - 1), (1, 0)):
            if passes:

                @pl.when((c == relay) & (i + AHEAD < chunks))
                def _():
                    ag_copy(i + AHEAD, c, end).start()

    def rs_copy(i, owner_g, owner_q, to_g, to_q):
        return pltpu.make_async_remote_copy(
            src_ref=outbox.at[i, to_q], dst_ref=inbox.at[i, owner_g * n_row + owner_q],
            send_sem=rs_send.at[i, to_q], recv_sem=rs_recv.at[i, owner_g * n_row + owner_q],
            device_id=(to_g, to_q, c), device_id_type=MESH,
        )

    def anc_copy(w, peer_g):
        return pltpu.make_async_remote_copy(
            src_ref=anc_box.at[w], dst_ref=anc_box.at[w],
            send_sem=anc_send.at[w, peer_g], recv_sem=anc_recv.at[w],
            device_id=(peer_g, q, c), device_id_type=MESH,
        )

    def full_dot(a, b):
        return jnp.dot(a, b, precision=lax.Precision.HIGHEST, preferred_element_type=jnp.float32)

    def solve(i, k, w, first):
        rest = rhs[k, :, cols(w)]
        if not first:
            back = i - chunks
            total = pending[w, (k - 1) * n_row + q]
            for d in range(1, n_row):
                other = lax.rem(q + d, n_row)
                rs_copy(back, g, other, g, q).wait_recv()
                total = total + inbox[back, g * n_row + other].astype(jnp.float32)
            rest = rest - total
        answer = full_dot(inv[k], rest)
        sub_out[k, :, cols(w)] = answer
        gathered[i, c] = answer.astype(jnp.bfloat16)

    def pass_on(arrived, onward):
        arrived.wait_recv()
        onward.start()

    def spread(i, k, w):
        for d in range(1, n_col):
            other = lax.rem(c + d, n_col)
            passed = False
            for owner, relay, end in passes:
                passed = passed | ((c == relay) & (other == owner))

            @pl.when(jnp.logical_not(passed))
            def _():
                ag_copy(i, other, c).wait_recv()

        for s in range(n_col):
            fetched[s] = gathered[i, s]

        for j in range(slots):
            product = jnp.dot(
                tiles[k, j], fetched[src_s[k * slots + j]], preferred_element_type=jnp.float32
            )
            chain[j + 1] = product + chain[prev_s[k * slots + j]]

        def updated(code):
            return pending[w, code] + chain[last_s[k * codes + code]]

        to_g = jnp.where(k < depth - 1, g, lax.rem(w, n_grp))
        for d in list(range(1, n_row)) + [0]:
            to_q = lax.rem(q + d, n_row)
            value = updated(k * n_row + to_q)

            def send():
                outbox[i, to_q] = value.astype(jnp.bfloat16)
                rs_copy(i, g, q, to_g, to_q).start()

            if d == 0:
                pending[w, k * n_row + q] = value
                pl.when(to_g != g)(send)
            else:
                send()

        def collect(code, carry):
            pending[w, code] = updated(code)
            return carry

        lax.fori_loop((k + 1) * n_row, codes, collect, 0)

    def finish(w):
        i = (depth - 1) * chunks + w

        @pl.when(lax.rem(w, n_grp) == g)
        def _():
            total = pending[w, (depth - 1) * n_row + q]
            for e in range(n_grp):
                for d in range(n_row):
                    if e or d:
                        other_g, other_q = lax.rem(g + e, n_grp), lax.rem(q + d, n_row)
                        rs_copy(i, other_g, other_q, g, q).wait_recv()
                        total = total + inbox[i, other_g * n_row + other_q].astype(jnp.float32)
            anc_box[w] = full_dot(anc_inv[...], anc_rhs[:, cols(w)] - total)
            for e in range(1, n_grp):
                anc_copy(w, lax.rem(g + e, n_grp)).start()

    for load in early:
        load.wait()
    for load in maps + loads:
        load.start()
    solve(0, 0, 0, True)
    pl.semaphore_wait(barrier, n_col - 1 + n_grp * n_row - 1 - strangers)

    send_direct(0)

    def first_level(w, carry):
        solve(w, 0, w, True)
        send_direct(w)
        return carry

    lax.fori_loop(1, chunks, first_level, 0)
    for load in maps:
        load.wait()
    lax.fori_loop(0, depth, tables, 0)
    chain[0] = jnp.zeros(chain.shape[1:], jnp.float32)

    def clear(n, carry):
        pending[n // codes, lax.rem(n, codes)] = jnp.zeros(pending.shape[2:], jnp.float32)
        return carry

    lax.fori_loop(0, chunks * codes, clear, 0)
    for load in loads:
        load.wait()

    def middle(i, carry):
        spread(i, i // chunks, lax.rem(i, chunks))

        @pl.when(i + 1 < steps)
        def _():
            relays(i + 1, pass_on)
            release(i + 1)

        later = i + chunks - LAG

        @pl.when((i >= LAG) & (later < steps))
        def _():
            solve(later, later // chunks, lax.rem(later, chunks), False)
            send_direct(later)

        @pl.when(later >= steps)
        def _():
            finish(later - steps)

        return carry

    relays(0, pass_on)
    release(0)
    lax.fori_loop(0, steps, middle, 0)
    for w in range(chunks - LAG, chunks):
        finish(jnp.int32(w))

    def deliver(w, carry):
        owner = lax.rem(w, n_grp)

        @pl.when(owner != g)
        def _():
            anc_copy(w, g).wait_recv()

        anc_out[:, cols(w)] = anc_box[w]

        @pl.when(owner == g)
        def _():
            for e in range(1, n_grp):
                anc_copy(w, lax.rem(g + e, n_grp)).wait_send()

        return carry

    lax.fori_loop(0, chunks, deliver, 0)

    def drain(i, carry):
        each_direct(i, lambda copy, wait_turn: copy.wait_send())
        relays(i, lambda arrived, onward: onward.wait_send())
        to_g = jnp.where(i < (depth - 1) * chunks, g, lax.rem(lax.rem(i, chunks), n_grp))
        for d in range(1, n_row):
            rs_copy(i, g, q, to_g, lax.rem(q + d, n_row)).wait_send()

        @pl.when(to_g != g)
        def _():
            rs_copy(i, g, q, to_g, q).wait_send()

        return carry

    lax.fori_loop(0, steps, drain, 0)


def hand_over(sub_ref, anc_ref, sub_out, anc_out, sem):
    copies = [
        pltpu.make_async_copy(sub_ref, sub_out, sem.at[0]),
        pltpu.make_async_copy(anc_ref, anc_out, sem.at[1]),
    ]
    for copy in copies:
        copy.start()
    for copy in copies:
        copy.wait()


def on_device(mesh, sub_rhs, sub_dinv, anc_rhs, anc_dinv, tiles, tile_target, tile_source, tile_count):
    n_grp, n_row, n_col = mesh.shape["grp"], mesh.shape["row"], mesh.shape["col"]
    depth, size, width = sub_rhs.shape[1], sub_rhs.shape[4], sub_rhs.shape[5]
    slots = tiles.shape[4]
    chunks = width // CHUNK
    steps = depth * chunks
    codes = depth * n_row
    bf16, f32 = jnp.bfloat16, jnp.float32
    dma = pltpu.SemaphoreType.DMA
    sub, anc = pl.pallas_call(
        functools.partial(kernel, n_grp, n_row, n_col),
        out_shape=(
            pltpu.VMEM((depth, size, width), f32),
            pltpu.VMEM((size, width), f32),
        ),
        in_specs=[pl.BlockSpec(memory_space=pltpu.HBM)] * 8,
        out_specs=(pl.BlockSpec(memory_space=pltpu.VMEM), pl.BlockSpec(memory_space=pltpu.VMEM)),
        scratch_shapes=[
            pltpu.VMEM((depth, size, width), f32),
            pltpu.VMEM((depth, size, size), f32),
            pltpu.VMEM((size, width), f32),
            pltpu.VMEM((size, size), f32),
            pltpu.VMEM((depth, slots, size, size), bf16),
            pltpu.VMEM((steps, n_col, size, CHUNK), bf16),
            pltpu.VMEM((n_col, size, CHUNK), bf16),
            pltpu.VMEM((slots + 1, size, CHUNK), f32),
            pltpu.VMEM((chunks, codes, size, CHUNK), f32),
            pltpu.VMEM((steps, n_row, size, CHUNK), bf16),
            pltpu.VMEM((steps, n_grp * n_row, size, CHUNK), bf16),
            pltpu.VMEM((chunks, size, CHUNK), f32),
            pltpu.SMEM((depth, 1, slots), jnp.int32),
            pltpu.SMEM((depth, 1, slots), jnp.int32),
            pltpu.SMEM((1, 1, 1, depth), jnp.int32),
            pltpu.SMEM((depth * slots,), jnp.int32),
            pltpu.SMEM((depth * codes,), jnp.int32),
            pltpu.SMEM((depth * slots,), jnp.int32),
            dma((10,)),
            dma((steps, n_col)),
            dma((steps, n_col)),
            dma((steps, max(len(hops(n_col)), 1))),
            dma((steps, n_row)),
            dma((steps, n_grp * n_row)),
            dma((chunks, n_grp)),
            dma((chunks,)),
        ],
        compiler_params=pltpu.CompilerParams(
            collective_id=0, has_side_effects=True, vmem_limit_bytes=67_043_328 - 4 * (depth + 1) * size * width
        ),
    )(
        tile_target.reshape(depth, 1, slots), tile_source.reshape(depth, 1, slots), tile_count,
        sub_rhs.reshape(depth, size, width), sub_dinv.reshape(depth, size, size),
        anc_rhs.reshape(size, width), anc_dinv.reshape(size, size),
        tiles.reshape(depth, slots, size, size),
    )
    sub, anc = pl.pallas_call(
        hand_over,
        out_shape=(
            jax.ShapeDtypeStruct((depth, size, width), f32),
            jax.ShapeDtypeStruct((size, width), f32),
        ),
        in_specs=[pl.BlockSpec(memory_space=pl.ANY)] * 2,
        out_specs=(pl.BlockSpec(memory_space=pl.ANY), pl.BlockSpec(memory_space=pl.ANY)),
        scratch_shapes=[dma((2,))],
        compiler_params=pltpu.CompilerParams(vmem_limit_bytes=1 << 20),
    )(sub, anc)
    return sub[None, :, None, None], anc[None, None]


def solution(mesh):
    placed = (
        P("grp", None, "row", "col", None, None),
        P("grp", None, "row", "col", None, None),
        P("row", "col", None, None),
        P("row", "col", None, None),
        P("grp", "row", "col", None, None, None, None),
        P("grp", "row", "col", None, None),
        P("grp", "row", "col", None, None),
        P("grp", "row", "col", None),
    )
    return jax.shard_map(
        functools.partial(on_device, mesh),
        mesh=mesh,
        in_specs=placed,
        out_specs=(P("grp", None, "row", "col", None, None), P("row", "col", None, None)),
        check_vma=False,
    )
```

```python
import functools

import jax
import jax.numpy as jnp
from jax import lax
from jax.experimental import pallas as pl
from jax.experimental.pallas import tpu as pltpu
from jax.sharding import PartitionSpec as P

MESH = pl.DeviceIdType.MESH
CHUNK = 128
AHEAD = 3
LAG = 1
BEHIND = 3


def hops(n_col):
    if not 2 < n_col <= 4:
        return ()
    up = [(o, n_col - 2, n_col - 1) for o in reversed(range(n_col - 2))]
    down = [(o, 1, 0) for o in range(2, n_col)]
    return tuple(up + down)


def kernel(
    n_grp, n_row, n_col,
    target_hbm, source_hbm, count_hbm,
    rhs_hbm, inv_hbm, anc_rhs_hbm, anc_inv_hbm, tiles_hbm,
    sub_out, anc_out,
    rhs, inv, anc_rhs, anc_inv, tiles,
    gathered, fetched, chain, pending, outbox, inbox, anc_box,
    target_ref, source_ref, count_ref, prev_s, last_s, src_s,
    load_sem, ag_send, ag_recv, fwd_send, rs_send, rs_recv, anc_send, anc_recv, plane_sem,
):
    depth, size, width = rhs.shape
    slots = tiles.shape[1]
    chunks = width // CHUNK
    steps = depth * chunks
    codes = depth * n_row
    passes = hops(n_col)
    g = lax.axis_index("grp")
    q = lax.axis_index("row")
    c = lax.axis_index("col")

    early = [
        pltpu.make_async_copy(inv_hbm.at[0], inv.at[0], load_sem.at[0]),
        pltpu.make_async_copy(rhs_hbm.at[0, :, pl.ds(0, CHUNK)], rhs.at[0, :, pl.ds(0, CHUNK)], load_sem.at[1]),
    ]
    others = pl.ds(CHUNK, width - CHUNK)
    second = pltpu.make_async_copy(rhs_hbm.at[0, :, others], rhs.at[0, :, others], load_sem.at[10])
    maps = [
        pltpu.make_async_copy(target_hbm, target_ref, load_sem.at[7]),
        pltpu.make_async_copy(source_hbm, source_ref, load_sem.at[8]),
        pltpu.make_async_copy(count_hbm, count_ref, load_sem.at[9]),
    ]
    loads = [
        pltpu.make_async_copy(tiles_hbm, tiles, load_sem.at[2]),
        pltpu.make_async_copy(anc_rhs_hbm, anc_rhs, load_sem.at[3]),
        pltpu.make_async_copy(anc_inv_hbm, anc_inv, load_sem.at[4]),
    ]
    if depth > 1:
        loads += [
            pltpu.make_async_copy(inv_hbm.at[pl.ds(1, depth - 1)], inv.at[pl.ds(1, depth - 1)], load_sem.at[5]),
            pltpu.make_async_copy(rhs_hbm.at[pl.ds(1, depth - 1)], rhs.at[pl.ds(1, depth - 1)], load_sem.at[6]),
        ]
    for load in early + [second]:
        load.start()

    barrier = pltpu.get_barrier_semaphore()
    targets = n_col - 1
    for owner, relay, end in passes:
        targets = targets - (c == owner).astype(jnp.int32)
    for d in range(1, n_col):
        peer = lax.rem(c + d, n_col)
        writes_here = True
        for owner, relay, end in passes:
            writes_here = writes_here & jnp.logical_not((peer == owner) & (c == end))

        @pl.when(writes_here)
        def _():
            pl.semaphore_signal(barrier, inc=1, device_id=(g, q, peer), device_id_type=MESH)

    leads = (g == n_grp - 1) & (q == n_row - 1)
    followers = n_grp * n_row - 1

    @pl.when(jnp.logical_not(leads))
    def _():
        pl.semaphore_signal(barrier, inc=1, device_id=(n_grp - 1, n_row - 1, c), device_id_type=MESH)

    def gather_plane():
        @pl.when(leads)
        def _():
            for e in range(n_grp):
                for d in range(n_row):
                    if e or d:
                        pl.semaphore_signal(
                            plane_sem, inc=1,
                            device_id=(lax.rem(g + e, n_grp), lax.rem(q + d, n_row), c), device_id_type=MESH,
                        )

    def await_plane():
        @pl.when(jnp.logical_not(leads))
        def _():
            pl.semaphore_wait(plane_sem, 1)

    def tables(k, carry):
        count = count_ref[0, 0, 0, k]
        raw = [target_ref[k, 0, j] for j in range(slots)]
        live = [jnp.where(j < count, raw[j], -1) for j in range(slots)]
        for j in range(slots):
            found = jnp.int32(0)
            for i in range(j):
                found = jnp.where(raw[i] == raw[j], i + 1, found)
            prev_s[k * slots + j] = found
            src_s[k * slots + j] = jnp.clip(source_ref[k, 0, j], 0, n_col - 1)
        for code in range(codes):
            found = jnp.int32(0)
            for j in range(slots):
                found = jnp.where(live[j] == code, j + 1, found)
            last_s[k * codes + code] = found
        return carry

    def cols(w):
        return pl.ds(pl.multiple_of(w * CHUNK, CHUNK), CHUNK)

    def ag_copy(i, owner, peer):
        return pltpu.make_async_remote_copy(
            src_ref=gathered.at[i, owner], dst_ref=gathered.at[i, owner],
            send_sem=ag_send.at[i, peer], recv_sem=ag_recv.at[i, owner],
            device_id=(g, q, peer), device_id_type=MESH,
        )

    def relays(i, run):
        for way, (owner, relay, end) in enumerate(passes):

            @pl.when(c == relay)
            def _():
                run(
                    ag_copy(i, owner, c),
                    pltpu.make_async_remote_copy(
                        src_ref=gathered.at[i, owner], dst_ref=gathered.at[i, owner],
                        send_sem=fwd_send.at[i, way], recv_sem=ag_recv.at[i, owner],
                        device_id=(g, q, end), device_id_type=MESH,
                    ),
                )

    def each_direct(i, run):
        for d in range(1, n_col):
            peer = lax.rem(c + d, n_col)
            far = False
            for owner, relay, end in passes:
                far = far | ((c == owner) & (peer == end))

            @pl.when(jnp.logical_not(far))
            def _():
                run(ag_copy(i, c, peer), held(i, peer))

    def held(i, peer):
        if not passes:
            return False
        to_end = ((c == n_col - 2) & (peer == n_col - 1)) | ((c == 1) & (peer == 0))
        return to_end & (i >= AHEAD) & (i < chunks)

    def send_direct(i):
        def start(copy, wait_turn):
            pl.when(jnp.logical_not(wait_turn))(copy.start)

        each_direct(i, start)

    def release(i):
        for relay, end in ((n_col - 2, n_col - 1), (1, 0)):
            if passes:

                @pl.when((c == relay) & (i + AHEAD < chunks))
                def _():
                    ag_copy(i + AHEAD, c, end).start()

    def rs_copy(i, owner_g, owner_q, to_g, to_q):
        return pltpu.make_async_remote_copy(
            src_ref=outbox.at[i, to_q], dst_ref=inbox.at[i, owner_g * n_row + owner_q],
            send_sem=rs_send.at[i, to_q], recv_sem=rs_recv.at[i, owner_g * n_row + owner_q],
            device_id=(to_g, to_q, c), device_id_type=MESH,
        )

    def anc_copy(w, peer_g):
        return pltpu.make_async_remote_copy(
            src_ref=anc_box.at[w], dst_ref=anc_box.at[w],
            send_sem=anc_send.at[w, peer_g], recv_sem=anc_recv.at[w],
            device_id=(peer_g, q, c), device_id_type=MESH,
        )

    def full_dot(a, b):
        return jnp.dot(a, b, precision=lax.Precision.HIGHEST, preferred_element_type=jnp.float32)

    def solve(i, k, w, first):
        rest = rhs[k, :, cols(w)]
        if not first:
            back = i - chunks
            total = pending[w, (k - 1) * n_row + q]
            for d in range(1, n_row):
                other = lax.rem(q + d, n_row)
                rs_copy(back, g, other, g, q).wait_recv()
                total = total + inbox[back, g * n_row + other].astype(jnp.float32)
            rest = rest - total
        answer = full_dot(inv[k], rest)
        sub_out[k, :, cols(w)] = answer
        gathered[i, c] = answer.astype(jnp.bfloat16)

    def pass_on(arrived, onward):
        arrived.wait_recv()
        onward.start()

    def spread(i, k, w):
        for d in range(1, n_col):
            other = lax.rem(c + d, n_col)
            passed = False
            for owner, relay, end in passes:
                passed = passed | ((c == relay) & (other == owner))

            @pl.when(jnp.logical_not(passed))
            def _():
                ag_copy(i, other, c).wait_recv()

        for s in range(n_col):
            fetched[s] = gathered[i, s]

        for j in range(slots):
            product = jnp.dot(
                tiles[k, j], fetched[src_s[k * slots + j]], preferred_element_type=jnp.float32
            )
            chain[j + 1] = product + chain[prev_s[k * slots + j]]

        def updated(code):
            return pending[w, code] + chain[last_s[k * codes + code]]

        to_g = jnp.where(k < depth - 1, g, lax.rem(w, n_grp))
        for d in list(range(1, n_row)) + [0]:
            to_q = lax.rem(q + d, n_row)
            value = updated(k * n_row + to_q)

            def send():
                outbox[i, to_q] = value.astype(jnp.bfloat16)
                rs_copy(i, g, q, to_g, to_q).start()

            if d == 0:
                pending[w, k * n_row + q] = value
                pl.when(to_g != g)(send)
            else:
                send()

        def collect(code, carry):
            pending[w, code] = updated(code)
            return carry

        lax.fori_loop((k + 1) * n_row, codes, collect, 0)

    def finish(w):
        i = (depth - 1) * chunks + w

        @pl.when(lax.rem(w, n_grp) == g)
        def _():
            total = pending[w, (depth - 1) * n_row + q]
            for e in range(n_grp):
                for d in range(n_row):
                    if e or d:
                        other_g, other_q = lax.rem(g + e, n_grp), lax.rem(q + d, n_row)
                        rs_copy(i, other_g, other_q, g, q).wait_recv()
                        total = total + inbox[i, other_g * n_row + other_q].astype(jnp.float32)
            anc_box[w] = full_dot(anc_inv[...], anc_rhs[:, cols(w)] - total)
            for e in range(1, n_grp):
                anc_copy(w, lax.rem(g + e, n_grp)).start()

    for load in early:
        load.wait()
    solve(0, 0, 0, True)
    pl.semaphore_wait(barrier, targets + jnp.where(leads, followers, 0))

    send_direct(0)
    second.wait()
    for load in maps + loads:
        load.start()

    def first_level(w, carry):
        solve(w, 0, w, True)
        send_direct(w)
        return carry

    lax.fori_loop(1, chunks, first_level, 0)
    gather_plane()
    for load in maps:
        load.wait()
    lax.fori_loop(0, depth, tables, 0)
    chain[0] = jnp.zeros(chain.shape[1:], jnp.float32)

    def clear(n, carry):
        pending[n // codes, lax.rem(n, codes)] = jnp.zeros(pending.shape[2:], jnp.float32)
        return carry

    lax.fori_loop(0, chunks * codes, clear, 0)
    for load in loads:
        load.wait()

    def middle(i, carry):
        spread(i, i // chunks, lax.rem(i, chunks))

        @pl.when(i + 1 < steps)
        def _():
            relays(i + 1, pass_on)
            release(i + 1)

        later = i + chunks - LAG

        @pl.when((i >= LAG) & (later < steps))
        def _():
            solve(later, later // chunks, lax.rem(later, chunks), False)
            send_direct(later)

        @pl.when(later >= steps)
        def _():
            finish(later - steps)

        pl.when(later > steps)(lambda: deliver(later - steps - 1))
        pl.when(i >= BEHIND)(lambda: drain(i - BEHIND))
        return carry

    def deliver(w):
        owner = lax.rem(w, n_grp)

        @pl.when(owner != g)
        def _():
            anc_copy(w, g).wait_recv()

        anc_out[:, cols(w)] = anc_box[w]

        @pl.when(owner == g)
        def _():
            for e in range(1, n_grp):
                anc_copy(w, lax.rem(g + e, n_grp)).wait_send()

    def drain(i):
        each_direct(i, lambda copy, wait_turn: copy.wait_send())
        relays(i, lambda arrived, onward: onward.wait_send())
        to_g = jnp.where(i < (depth - 1) * chunks, g, lax.rem(lax.rem(i, chunks), n_grp))
        for d in range(1, n_row):
            rs_copy(i, g, q, to_g, lax.rem(q + d, n_row)).wait_send()

        @pl.when(to_g != g)
        def _():
            rs_copy(i, g, q, to_g, q).wait_send()

    await_plane()
    relays(0, pass_on)
    release(0)
    lax.fori_loop(0, steps, middle, 0)
    for w in range(chunks - LAG, chunks):
        finish(jnp.int32(w))
    for i in range(steps - BEHIND, steps):
        drain(jnp.int32(i))
    for w in range(chunks - LAG - 1, chunks):
        deliver(jnp.int32(w))


def hand_over(sub_ref, anc_ref, sub_out, anc_out, sem):
    copies = [
        pltpu.make_async_copy(sub_ref, sub_out, sem.at[0]),
        pltpu.make_async_copy(anc_ref, anc_out, sem.at[1]),
    ]
    for copy in copies:
        copy.start()
    for copy in copies:
        copy.wait()


def on_device(mesh, sub_rhs, sub_dinv, anc_rhs, anc_dinv, tiles, tile_target, tile_source, tile_count):
    n_grp, n_row, n_col = mesh.shape["grp"], mesh.shape["row"], mesh.shape["col"]
    depth, size, width = sub_rhs.shape[1], sub_rhs.shape[4], sub_rhs.shape[5]
    slots = tiles.shape[4]
    chunks = width // CHUNK
    steps = depth * chunks
    codes = depth * n_row
    bf16, f32 = jnp.bfloat16, jnp.float32
    dma = pltpu.SemaphoreType.DMA
    sub, anc = pl.pallas_call(
        functools.partial(kernel, n_grp, n_row, n_col),
        out_shape=(
            pltpu.VMEM((depth, size, width), f32),
            pltpu.VMEM((size, width), f32),
        ),
        in_specs=[pl.BlockSpec(memory_space=pltpu.HBM)] * 8,
        out_specs=(pl.BlockSpec(memory_space=pltpu.VMEM), pl.BlockSpec(memory_space=pltpu.VMEM)),
        scratch_shapes=[
            pltpu.VMEM((depth, size, width), f32),
            pltpu.VMEM((depth, size, size), f32),
            pltpu.VMEM((size, width), f32),
            pltpu.VMEM((size, size), f32),
            pltpu.VMEM((depth, slots, size, size), bf16),
            pltpu.VMEM((steps, n_col, size, CHUNK), bf16),
            pltpu.VMEM((n_col, size, CHUNK), bf16),
            pltpu.VMEM((slots + 1, size, CHUNK), f32),
            pltpu.VMEM((chunks, codes, size, CHUNK), f32),
            pltpu.VMEM((steps, n_row, size, CHUNK), bf16),
            pltpu.VMEM((steps, n_grp * n_row, size, CHUNK), bf16),
            pltpu.VMEM((chunks, size, CHUNK), f32),
            pltpu.SMEM((depth, 1, slots), jnp.int32),
            pltpu.SMEM((depth, 1, slots), jnp.int32),
            pltpu.SMEM((1, 1, 1, depth), jnp.int32),
            pltpu.SMEM((depth * slots,), jnp.int32),
            pltpu.SMEM((depth * codes,), jnp.int32),
            pltpu.SMEM((depth * slots,), jnp.int32),
            dma((11,)),
            dma((steps, n_col)),
            dma((steps, n_col)),
            dma((steps, max(len(hops(n_col)), 1))),
            dma((steps, n_row)),
            dma((steps, n_grp * n_row)),
            dma((chunks, n_grp)),
            dma((chunks,)),
            pltpu.SemaphoreType.REGULAR,
        ],
        compiler_params=pltpu.CompilerParams(
            collective_id=0, has_side_effects=True, vmem_limit_bytes=67_043_328 - 4 * (depth + 1) * size * width
        ),
    )(
        tile_target.reshape(depth, 1, slots), tile_source.reshape(depth, 1, slots), tile_count,
        sub_rhs.reshape(depth, size, width), sub_dinv.reshape(depth, size, size),
        anc_rhs.reshape(size, width), anc_dinv.reshape(size, size),
        tiles.reshape(depth, slots, size, size),
    )
    sub, anc = pl.pallas_call(
        hand_over,
        out_shape=(
            jax.ShapeDtypeStruct((depth, size, width), f32),
            jax.ShapeDtypeStruct((size, width), f32),
        ),
        in_specs=[pl.BlockSpec(memory_space=pl.ANY)] * 2,
        out_specs=(pl.BlockSpec(memory_space=pl.ANY), pl.BlockSpec(memory_space=pl.ANY)),
        scratch_shapes=[dma((2,))],
        compiler_params=pltpu.CompilerParams(vmem_limit_bytes=1 << 20),
    )(sub, anc)
    return sub[None, :, None, None], anc[None, None]


def solution(mesh):
    placed = (
        P("grp", None, "row", "col", None, None),
        P("grp", None, "row", "col", None, None),
        P("row", "col", None, None),
        P("row", "col", None, None),
        P("grp", "row", "col", None, None, None, None),
        P("grp", "row", "col", None, None),
        P("grp", "row", "col", None, None),
        P("grp", "row", "col", None),
    )
    return jax.shard_map(
        functools.partial(on_device, mesh),
        mesh=mesh,
        in_specs=placed,
        out_specs=(P("grp", None, "row", "col", None, None), P("row", "col", None, None)),
        check_vma=False,
    )
```

```python
import functools

import jax
import jax.numpy as jnp
from jax import lax
from jax.experimental import pallas as pl
from jax.experimental.pallas import tpu as pltpu
from jax.sharding import PartitionSpec as P

MESH = pl.DeviceIdType.MESH
CHUNK = 128
AHEAD = 3
LAG = 1
BEHIND = 3


def hops(n_col):
    if not 2 < n_col <= 4:
        return ()
    up = [(o, n_col - 2, n_col - 1) for o in reversed(range(n_col - 2))]
    down = [(o, 1, 0) for o in range(2, n_col)]
    return tuple(up + down)


def kernel(
    n_grp, n_row, n_col,
    target_hbm, source_hbm, count_hbm,
    rhs_hbm, inv_hbm, anc_rhs_hbm, anc_inv_hbm, tiles_hbm,
    sub_out, anc_out,
    rhs, inv, anc_rhs, anc_inv, tiles,
    gathered, fetched, chain, pending, outbox, inbox, anc_box,
    target_ref, source_ref, count_ref, prev_s, last_s, src_s,
    load_sem, ag_send, ag_recv, fwd_send, rs_send, rs_recv, anc_send, anc_recv, plane_sem,
):
    depth, size, width = rhs.shape
    slots = tiles.shape[1]
    chunks = width // CHUNK
    steps = depth * chunks
    codes = depth * n_row
    passes = hops(n_col)
    g = lax.axis_index("grp")
    q = lax.axis_index("row")
    c = lax.axis_index("col")

    early = [
        pltpu.make_async_copy(inv_hbm.at[0], inv.at[0], load_sem.at[0]),
        pltpu.make_async_copy(rhs_hbm.at[0, :, pl.ds(0, CHUNK)], rhs.at[0, :, pl.ds(0, CHUNK)], load_sem.at[1]),
    ]
    others = pl.ds(CHUNK, width - CHUNK)
    second = pltpu.make_async_copy(rhs_hbm.at[0, :, others], rhs.at[0, :, others], load_sem.at[10])
    maps = [
        pltpu.make_async_copy(target_hbm, target_ref, load_sem.at[7]),
        pltpu.make_async_copy(source_hbm, source_ref, load_sem.at[8]),
        pltpu.make_async_copy(count_hbm, count_ref, load_sem.at[9]),
    ]
    loads = [
        pltpu.make_async_copy(tiles_hbm, tiles, load_sem.at[2]),
        pltpu.make_async_copy(anc_rhs_hbm, anc_rhs, load_sem.at[3]),
        pltpu.make_async_copy(anc_inv_hbm, anc_inv, load_sem.at[4]),
    ]
    if depth > 1:
        loads += [
            pltpu.make_async_copy(inv_hbm.at[pl.ds(1, depth - 1)], inv.at[pl.ds(1, depth - 1)], load_sem.at[5]),
            pltpu.make_async_copy(rhs_hbm.at[pl.ds(1, depth - 1)], rhs.at[pl.ds(1, depth - 1)], load_sem.at[6]),
        ]
    for load in early + [second]:
        load.start()

    barrier = pltpu.get_barrier_semaphore()
    targets = n_col - 1
    for owner, relay, end in passes:
        targets = targets - (c == owner).astype(jnp.int32)
    for d in range(1, n_col):
        peer = lax.rem(c + d, n_col)
        writes_here = True
        for owner, relay, end in passes:
            writes_here = writes_here & jnp.logical_not((peer == owner) & (c == end))

        @pl.when(writes_here)
        def _():
            pl.semaphore_signal(barrier, inc=1, device_id=(g, q, peer), device_id_type=MESH)

    leads = (g == n_grp - 1) & (q == n_row - 1)
    followers = n_grp * n_row - 1

    @pl.when(jnp.logical_not(leads))
    def _():
        pl.semaphore_signal(barrier, inc=1, device_id=(n_grp - 1, n_row - 1, c), device_id_type=MESH)

    def gather_plane():
        @pl.when(leads)
        def _():
            for e in range(n_grp):
                for d in range(n_row):
                    if e or d:
                        pl.semaphore_signal(
                            plane_sem, inc=1,
                            device_id=(lax.rem(g + e, n_grp), lax.rem(q + d, n_row), c), device_id_type=MESH,
                        )

    def await_plane():
        @pl.when(jnp.logical_not(leads))
        def _():
            pl.semaphore_wait(plane_sem, 1)

    def tables(k, carry):
        count = count_ref[0, 0, 0, k]
        raw = [target_ref[k, 0, j] for j in range(slots)]
        live = [jnp.where(j < count, raw[j], -1) for j in range(slots)]
        for j in range(slots):
            found = jnp.int32(0)
            for i in range(j):
                found = jnp.where(raw[i] == raw[j], i + 1, found)
            prev_s[k * slots + j] = found
            src_s[k * slots + j] = jnp.clip(source_ref[k, 0, j], 0, n_col - 1)
        for code in range(codes):
            found = jnp.int32(0)
            for j in range(slots):
                found = jnp.where(live[j] == code, j + 1, found)
            last_s[k * codes + code] = found
        return carry

    def cols(w):
        return pl.ds(pl.multiple_of(w * CHUNK, CHUNK), CHUNK)

    def ag_copy(i, owner, peer):
        return pltpu.make_async_remote_copy(
            src_ref=gathered.at[i, owner], dst_ref=gathered.at[i, owner],
            send_sem=ag_send.at[i, peer], recv_sem=ag_recv.at[i, owner],
            device_id=(g, q, peer), device_id_type=MESH,
        )

    def relays(i, run):
        for way, (owner, relay, end) in enumerate(passes):

            @pl.when(c == relay)
            def _():
                run(
                    ag_copy(i, owner, c),
                    pltpu.make_async_remote_copy(
                        src_ref=gathered.at[i, owner], dst_ref=gathered.at[i, owner],
                        send_sem=fwd_send.at[i, way], recv_sem=ag_recv.at[i, owner],
                        device_id=(g, q, end), device_id_type=MESH,
                    ),
                )

    def each_direct(i, run):
        for d in range(1, n_col):
            peer = lax.rem(c + d, n_col)
            far = False
            for owner, relay, end in passes:
                far = far | ((c == owner) & (peer == end))

            @pl.when(jnp.logical_not(far))
            def _():
                run(ag_copy(i, c, peer), held(i, peer))

    def held(i, peer):
        if not passes:
            return False
        to_end = ((c == n_col - 2) & (peer == n_col - 1)) | ((c == 1) & (peer == 0))
        return to_end & (i >= AHEAD) & (i < chunks)

    def send_direct(i):
        def start(copy, wait_turn):
            pl.when(jnp.logical_not(wait_turn))(copy.start)

        each_direct(i, start)

    def release(i):
        for relay, end in ((n_col - 2, n_col - 1), (1, 0)):
            if passes:

                @pl.when((c == relay) & (i + AHEAD < chunks))
                def _():
                    ag_copy(i + AHEAD, c, end).start()

    def rs_copy(i, owner_g, owner_q, to_g, to_q):
        return pltpu.make_async_remote_copy(
            src_ref=outbox.at[i, to_q], dst_ref=inbox.at[i, owner_g * n_row + owner_q],
            send_sem=rs_send.at[i, to_q], recv_sem=rs_recv.at[i, owner_g * n_row + owner_q],
            device_id=(to_g, to_q, c), device_id_type=MESH,
        )

    def anc_copy(w, peer_g):
        return pltpu.make_async_remote_copy(
            src_ref=anc_box.at[w], dst_ref=anc_box.at[w],
            send_sem=anc_send.at[w, peer_g], recv_sem=anc_recv.at[w],
            device_id=(peer_g, q, c), device_id_type=MESH,
        )

    def full_dot(a, b):
        return jnp.dot(a, b, precision=lax.Precision.HIGHEST, preferred_element_type=jnp.float32)

    def solve(i, k, w, first):
        rest = rhs[k, :, cols(w)]
        if not first:
            back = i - chunks
            total = pending[w, (k - 1) * n_row + q]
            for d in range(1, n_row):
                other = lax.rem(q + d, n_row)
                rs_copy(back, g, other, g, q).wait_recv()
                total = total + inbox[back, g * n_row + other].astype(jnp.float32)
            rest = rest - total
        answer = full_dot(inv[k], rest)
        sub_out[k, :, cols(w)] = answer
        gathered[i, c] = answer.astype(jnp.bfloat16)

    def pass_on(arrived, onward):
        arrived.wait_recv()
        onward.start()

    def spread(i, k, w):
        for d in range(1, n_col):
            other = lax.rem(c + d, n_col)
            passed = False
            for owner, relay, end in passes:
                passed = passed | ((c == relay) & (other == owner))

            @pl.when(jnp.logical_not(passed))
            def _():
                ag_copy(i, other, c).wait_recv()

        for s in range(n_col):
            fetched[s] = gathered[i, s]

        for j in range(slots):
            product = jnp.dot(
                tiles[k, j], fetched[src_s[k * slots + j]], preferred_element_type=jnp.float32
            )
            chain[j + 1] = product + chain[prev_s[k * slots + j]]

        def updated(code):
            return pending[w, code] + chain[last_s[k * codes + code]]

        to_g = jnp.where(k < depth - 1, g, lax.rem(w, n_grp))
        for d in list(range(1, n_row)) + [0]:
            to_q = lax.rem(q + d, n_row)
            value = updated(k * n_row + to_q)

            def send():
                outbox[i, to_q] = value.astype(jnp.bfloat16)
                rs_copy(i, g, q, to_g, to_q).start()

            if d == 0:
                pending[w, k * n_row + q] = value
                pl.when(to_g != g)(send)
            else:
                send()

        def collect(code, carry):
            pending[w, code] = updated(code)
            return carry

        lax.fori_loop((k + 1) * n_row, codes, collect, 0)

    def finish(w):
        i = (depth - 1) * chunks + w

        @pl.when(lax.rem(w, n_grp) == g)
        def _():
            total = pending[w, (depth - 1) * n_row + q]
            for e in range(n_grp):
                for d in range(n_row):
                    if e or d:
                        other_g, other_q = lax.rem(g + e, n_grp), lax.rem(q + d, n_row)
                        rs_copy(i, other_g, other_q, g, q).wait_recv()
                        total = total + inbox[i, other_g * n_row + other_q].astype(jnp.float32)
            anc_box[w] = full_dot(anc_inv[...], anc_rhs[:, cols(w)] - total)
            for e in range(1, n_grp):
                anc_copy(w, lax.rem(g + e, n_grp)).start()

    for load in early:
        load.wait()
    solve(0, 0, 0, True)
    pl.semaphore_wait(barrier, targets + jnp.where(leads, followers, 0))

    send_direct(0)
    second.wait()
    for load in maps + loads:
        load.start()

    def first_level(w, carry):
        solve(w, 0, w, True)
        send_direct(w)
        return carry

    lax.fori_loop(1, chunks, first_level, 0)
    gather_plane()
    for load in maps:
        load.wait()
    lax.fori_loop(0, depth, tables, 0)
    chain[0] = jnp.zeros(chain.shape[1:], jnp.float32)

    def clear(n, carry):
        pending[n // codes, lax.rem(n, codes)] = jnp.zeros(pending.shape[2:], jnp.float32)
        return carry

    lax.fori_loop(0, chunks * codes, clear, 0)
    for load in loads:
        load.wait()

    def middle(i, carry):
        spread(i, i // chunks, lax.rem(i, chunks))

        @pl.when(i + 1 < steps)
        def _():
            relays(i + 1, pass_on)
            release(i + 1)

        later = i + chunks - LAG

        @pl.when((i >= LAG) & (later < steps))
        def _():
            solve(later, later // chunks, lax.rem(later, chunks), False)
            send_direct(later)

        @pl.when(later >= steps + 1)
        def _():
            finish(later - steps - 1)

        pl.when(later >= steps + 3)(lambda: deliver(later - steps - 3))
        pl.when(i >= BEHIND)(lambda: drain(i - BEHIND))
        return carry

    def deliver(w):
        owner = lax.rem(w, n_grp)

        @pl.when(owner != g)
        def _():
            anc_copy(w, g).wait_recv()

        anc_out[:, cols(w)] = anc_box[w]

        @pl.when(owner == g)
        def _():
            for e in range(1, n_grp):
                anc_copy(w, lax.rem(g + e, n_grp)).wait_send()

    def drain(i):
        each_direct(i, lambda copy, wait_turn: copy.wait_send())
        relays(i, lambda arrived, onward: onward.wait_send())
        to_g = jnp.where(i < (depth - 1) * chunks, g, lax.rem(lax.rem(i, chunks), n_grp))
        for d in range(1, n_row):
            rs_copy(i, g, q, to_g, lax.rem(q + d, n_row)).wait_send()

        @pl.when(to_g != g)
        def _():
            rs_copy(i, g, q, to_g, q).wait_send()

    await_plane()
    relays(0, pass_on)
    release(0)
    lax.fori_loop(0, steps, middle, 0)
    for w in range(max(chunks - LAG - 1, 0), chunks):
        finish(jnp.int32(w))
    for i in range(steps - BEHIND, steps):
        drain(jnp.int32(i))
    for w in range(max(chunks - LAG - 3, 0), chunks):
        deliver(jnp.int32(w))


def hand_over(sub_ref, anc_ref, sub_out, anc_out, sem):
    copies = [
        pltpu.make_async_copy(sub_ref, sub_out, sem.at[0]),
        pltpu.make_async_copy(anc_ref, anc_out, sem.at[1]),
    ]
    for copy in copies:
        copy.start()
    for copy in copies:
        copy.wait()


def on_device(mesh, sub_rhs, sub_dinv, anc_rhs, anc_dinv, tiles, tile_target, tile_source, tile_count):
    n_grp, n_row, n_col = mesh.shape["grp"], mesh.shape["row"], mesh.shape["col"]
    depth, size, width = sub_rhs.shape[1], sub_rhs.shape[4], sub_rhs.shape[5]
    slots = tiles.shape[4]
    chunks = width // CHUNK
    steps = depth * chunks
    codes = depth * n_row
    bf16, f32 = jnp.bfloat16, jnp.float32
    dma = pltpu.SemaphoreType.DMA
    sub, anc = pl.pallas_call(
        functools.partial(kernel, n_grp, n_row, n_col),
        out_shape=(
            pltpu.VMEM((depth, size, width), f32),
            pltpu.VMEM((size, width), f32),
        ),
        in_specs=[pl.BlockSpec(memory_space=pltpu.HBM)] * 8,
        out_specs=(pl.BlockSpec(memory_space=pltpu.VMEM), pl.BlockSpec(memory_space=pltpu.VMEM)),
        scratch_shapes=[
            pltpu.VMEM((depth, size, width), f32),
            pltpu.VMEM((depth, size, size), f32),
            pltpu.VMEM((size, width), f32),
            pltpu.VMEM((size, size), f32),
            pltpu.VMEM((depth, slots, size, size), bf16),
            pltpu.VMEM((steps, n_col, size, CHUNK), bf16),
            pltpu.VMEM((n_col, size, CHUNK), bf16),
            pltpu.VMEM((slots + 1, size, CHUNK), f32),
            pltpu.VMEM((chunks, codes, size, CHUNK), f32),
            pltpu.VMEM((steps, n_row, size, CHUNK), bf16),
            pltpu.VMEM((steps, n_grp * n_row, size, CHUNK), bf16),
            pltpu.VMEM((chunks, size, CHUNK), f32),
            pltpu.SMEM((depth, 1, slots), jnp.int32),
            pltpu.SMEM((depth, 1, slots), jnp.int32),
            pltpu.SMEM((1, 1, 1, depth), jnp.int32),
            pltpu.SMEM((depth * slots,), jnp.int32),
            pltpu.SMEM((depth * codes,), jnp.int32),
            pltpu.SMEM((depth * slots,), jnp.int32),
            dma((11,)),
            dma((steps, n_col)),
            dma((steps, n_col)),
            dma((steps, max(len(hops(n_col)), 1))),
            dma((steps, n_row)),
            dma((steps, n_grp * n_row)),
            dma((chunks, n_grp)),
            dma((chunks,)),
            pltpu.SemaphoreType.REGULAR,
        ],
        compiler_params=pltpu.CompilerParams(
            collective_id=0, has_side_effects=True, vmem_limit_bytes=67_043_328 - 4 * (depth + 1) * size * width
        ),
    )(
        tile_target.reshape(depth, 1, slots), tile_source.reshape(depth, 1, slots), tile_count,
        sub_rhs.reshape(depth, size, width), sub_dinv.reshape(depth, size, size),
        anc_rhs.reshape(size, width), anc_dinv.reshape(size, size),
        tiles.reshape(depth, slots, size, size),
    )
    sub, anc = pl.pallas_call(
        hand_over,
        out_shape=(
            jax.ShapeDtypeStruct((depth, size, width), f32),
            jax.ShapeDtypeStruct((size, width), f32),
        ),
        in_specs=[pl.BlockSpec(memory_space=pl.ANY)] * 2,
        out_specs=(pl.BlockSpec(memory_space=pl.ANY), pl.BlockSpec(memory_space=pl.ANY)),
        scratch_shapes=[dma((2,))],
        compiler_params=pltpu.CompilerParams(vmem_limit_bytes=1 << 20),
    )(sub, anc)
    return sub[None, :, None, None], anc[None, None]


def solution(mesh):
    placed = (
        P("grp", None, "row", "col", None, None),
        P("grp", None, "row", "col", None, None),
        P("row", "col", None, None),
        P("row", "col", None, None),
        P("grp", "row", "col", None, None, None, None),
        P("grp", "row", "col", None, None),
        P("grp", "row", "col", None, None),
        P("grp", "row", "col", None),
    )
    return jax.shard_map(
        functools.partial(on_device, mesh),
        mesh=mesh,
        in_specs=placed,
        out_specs=(P("grp", None, "row", "col", None, None), P("row", "col", None, None)),
        check_vma=False,
    )
```

```python
import functools

import jax
import jax.numpy as jnp
from jax import lax
from jax.experimental import pallas as pl
from jax.experimental.pallas import tpu as pltpu
from jax.sharding import PartitionSpec as P

MESH = pl.DeviceIdType.MESH
CHUNK = 128
AHEAD = 3
LAG = 1
BEHIND = 3


def hops(n_col):
    if not 2 < n_col <= 4:
        return ()
    up = [(o, n_col - 2, n_col - 1) for o in reversed(range(n_col - 2))]
    down = [(o, 1, 0) for o in range(2, n_col)]
    return tuple(up + down)


def kernel(
    n_grp, n_row, n_col,
    target_hbm, source_hbm, count_hbm,
    rhs_hbm, inv_hbm, anc_rhs_hbm, anc_inv_hbm, tiles_hbm,
    sub_out, anc_out,
    rhs, inv, anc_rhs, anc_inv, tiles, wide,
    gathered, fetched, chain, pending, outbox, inbox, anc_box,
    target_ref, source_ref, count_ref, prev_s, last_s, src_s,
    load_sem, ag_send, ag_recv, fwd_send, rs_send, rs_recv, anc_send, anc_recv, plane_sem,
):
    depth, size, width = rhs.shape
    slots = tiles.shape[1]
    chunks = width // CHUNK
    steps = depth * chunks
    codes = depth * n_row
    passes = hops(n_col)
    g = lax.axis_index("grp")
    q = lax.axis_index("row")
    c = lax.axis_index("col")

    early = [
        pltpu.make_async_copy(inv_hbm.at[0], inv.at[0], load_sem.at[0]),
        pltpu.make_async_copy(rhs_hbm.at[0, :, pl.ds(0, CHUNK)], rhs.at[0, :, pl.ds(0, CHUNK)], load_sem.at[1]),
    ]
    others = pl.ds(CHUNK, width - CHUNK)
    second = pltpu.make_async_copy(rhs_hbm.at[0, :, others], rhs.at[0, :, others], load_sem.at[10])
    maps = [
        pltpu.make_async_copy(target_hbm, target_ref, load_sem.at[7]),
        pltpu.make_async_copy(source_hbm, source_ref, load_sem.at[8]),
        pltpu.make_async_copy(count_hbm, count_ref, load_sem.at[9]),
    ]
    loads = [
        pltpu.make_async_copy(tiles_hbm, tiles, load_sem.at[2]),
        pltpu.make_async_copy(anc_rhs_hbm, anc_rhs, load_sem.at[3]),
        pltpu.make_async_copy(anc_inv_hbm, anc_inv, load_sem.at[4]),
    ]
    if depth > 1:
        loads += [
            pltpu.make_async_copy(inv_hbm.at[pl.ds(1, depth - 1)], inv.at[pl.ds(1, depth - 1)], load_sem.at[5]),
            pltpu.make_async_copy(rhs_hbm.at[pl.ds(1, depth - 1)], rhs.at[pl.ds(1, depth - 1)], load_sem.at[6]),
        ]
    for load in early + [second]:
        load.start()

    barrier = pltpu.get_barrier_semaphore()
    targets = n_col - 1
    for owner, relay, end in passes:
        targets = targets - (c == owner).astype(jnp.int32)
    for d in range(1, n_col):
        peer = lax.rem(c + d, n_col)
        writes_here = True
        for owner, relay, end in passes:
            writes_here = writes_here & jnp.logical_not((peer == owner) & (c == end))

        @pl.when(writes_here)
        def _():
            pl.semaphore_signal(barrier, inc=1, device_id=(g, q, peer), device_id_type=MESH)

    leads = (g == 0) & (q == n_row - 1)
    followers = n_grp * n_row - 1

    @pl.when(jnp.logical_not(leads))
    def _():
        pl.semaphore_signal(barrier, inc=1, device_id=(0, n_row - 1, c), device_id_type=MESH)

    def gather_plane():
        @pl.when(leads)
        def _():
            for e in range(n_grp):
                for d in range(n_row):
                    if e or d:
                        pl.semaphore_signal(
                            plane_sem, inc=1,
                            device_id=(lax.rem(g + e, n_grp), lax.rem(q + d, n_row), c), device_id_type=MESH,
                        )

    def await_plane():
        @pl.when(jnp.logical_not(leads))
        def _():
            pl.semaphore_wait(plane_sem, 1)

    def tables(k, carry):
        count = count_ref[0, 0, 0, k]
        raw = [target_ref[k, 0, j] for j in range(slots)]
        live = [jnp.where(j < count, raw[j], -1) for j in range(slots)]
        for j in range(slots):
            found = jnp.int32(0)
            for i in range(j):
                found = jnp.where(raw[i] == raw[j], i + 1, found)
            prev_s[k * slots + j] = found
            src_s[k * slots + j] = jnp.clip(source_ref[k, 0, j], 0, n_col - 1)
        for code in range(codes):
            found = jnp.int32(0)
            for j in range(slots):
                found = jnp.where(live[j] == code, j + 1, found)
            last_s[k * codes + code] = found
        return carry

    def cols(w):
        return pl.ds(pl.multiple_of(w * CHUNK, CHUNK), CHUNK)

    def ag_copy(i, owner, peer):
        return pltpu.make_async_remote_copy(
            src_ref=gathered.at[i, owner], dst_ref=gathered.at[i, owner],
            send_sem=ag_send.at[i, peer], recv_sem=ag_recv.at[i, owner],
            device_id=(g, q, peer), device_id_type=MESH,
        )

    def relays(i, run):
        for way, (owner, relay, end) in enumerate(passes):

            @pl.when(c == relay)
            def _():
                run(
                    ag_copy(i, owner, c),
                    pltpu.make_async_remote_copy(
                        src_ref=gathered.at[i, owner], dst_ref=gathered.at[i, owner],
                        send_sem=fwd_send.at[i, way], recv_sem=ag_recv.at[i, owner],
                        device_id=(g, q, end), device_id_type=MESH,
                    ),
                )

    def each_direct(i, run):
        for d in range(1, n_col):
            peer = lax.rem(c + d, n_col)
            far = False
            for owner, relay, end in passes:
                far = far | ((c == owner) & (peer == end))

            @pl.when(jnp.logical_not(far))
            def _():
                run(ag_copy(i, c, peer), held(i, peer))

    def held(i, peer):
        if not passes:
            return False
        to_end = ((c == n_col - 2) & (peer == n_col - 1)) | ((c == 1) & (peer == 0))
        return to_end & (i >= AHEAD) & (i < chunks)

    def send_direct(i):
        def start(copy, wait_turn):
            pl.when(jnp.logical_not(wait_turn))(copy.start)

        each_direct(i, start)

    def release(i):
        for relay, end in ((n_col - 2, n_col - 1), (1, 0)):
            if passes:

                @pl.when((c == relay) & (i + AHEAD < chunks))
                def _():
                    ag_copy(i + AHEAD, c, end).start()

    def rs_copy(i, owner_g, owner_q, to_g, to_q):
        return pltpu.make_async_remote_copy(
            src_ref=outbox.at[i, to_q], dst_ref=inbox.at[i, owner_g * n_row + owner_q],
            send_sem=rs_send.at[i, to_q], recv_sem=rs_recv.at[i, owner_g * n_row + owner_q],
            device_id=(to_g, to_q, c), device_id_type=MESH,
        )

    def anc_copy(w, peer_g):
        return pltpu.make_async_remote_copy(
            src_ref=anc_box.at[w], dst_ref=anc_box.at[w],
            send_sem=anc_send.at[w, peer_g], recv_sem=anc_recv.at[w],
            device_id=(peer_g, q, c), device_id_type=MESH,
        )

    def full_dot(a, b):
        high = b.astype(jnp.bfloat16)
        low = (b - high.astype(jnp.float32)).astype(jnp.bfloat16)
        return jnp.dot(a, jnp.concatenate([high, low, high], axis=0), preferred_element_type=jnp.float32)

    def widen(a):
        high = a.astype(jnp.bfloat16)
        low = (a - high.astype(jnp.float32)).astype(jnp.bfloat16)
        return jnp.concatenate([high, high, low], axis=1)

    def solve(i, k, w, first):
        rest = rhs[k, :, cols(w)]
        if not first:
            back = i - chunks
            total = pending[w, (k - 1) * n_row + q]
            for d in range(1, n_row):
                other = lax.rem(q + d, n_row)
                rs_copy(back, g, other, g, q).wait_recv()
                total = total + inbox[back, g * n_row + other].astype(jnp.float32)
            rest = rest - total
        answer = full_dot(wide[k], rest)
        sub_out[k, :, cols(w)] = answer
        gathered[i, c] = answer.astype(jnp.bfloat16)

    def pass_on(arrived, onward):
        arrived.wait_recv()
        onward.start()

    def spread(i, k, w):
        fetched[c] = gathered[i, c]
        for d in range(1, n_col):
            other = lax.rem(c + jnp.where(c < n_col // 2, d, n_col - d), n_col)
            passed = False
            for owner, relay, end in passes:
                passed = passed | ((c == relay) & (other == owner))

            @pl.when(jnp.logical_not(passed))
            def _():
                ag_copy(i, other, c).wait_recv()

            fetched[other] = gathered[i, other]

        for j in range(slots):
            product = jnp.dot(
                tiles[k, j], fetched[src_s[k * slots + j]], preferred_element_type=jnp.float32
            )
            chain[j + 1] = product + chain[prev_s[k * slots + j]]

        def updated(code):
            return pending[w, code] + chain[last_s[k * codes + code]]

        to_g = jnp.where(k < depth - 1, g, lax.rem(w, n_grp))
        for d in list(range(1, n_row)) + [0]:
            to_q = lax.rem(q + d, n_row)
            value = updated(k * n_row + to_q)

            def send():
                outbox[i, to_q] = value.astype(jnp.bfloat16)
                rs_copy(i, g, q, to_g, to_q).start()

            if d == 0:
                pending[w, k * n_row + q] = value
                pl.when(to_g != g)(send)
            else:
                send()

        def collect(code, carry):
            pending[w, code] = updated(code)
            return carry

        lax.fori_loop((k + 1) * n_row, codes, collect, 0)

    def finish(w):
        i = (depth - 1) * chunks + w

        @pl.when(lax.rem(w, n_grp) == g)
        def _():
            total = pending[w, (depth - 1) * n_row + q]
            for e in range(n_grp):
                for d in range(n_row):
                    if e or d:
                        other_g, other_q = lax.rem(g + e, n_grp), lax.rem(q + d, n_row)
                        rs_copy(i, other_g, other_q, g, q).wait_recv()
                        total = total + inbox[i, other_g * n_row + other_q].astype(jnp.float32)
            anc_box[w] = full_dot(wide[depth], anc_rhs[:, cols(w)] - total)
            for e in range(1, n_grp):
                anc_copy(w, lax.rem(g + e, n_grp)).start()

    for load in early:
        load.wait()
    wide[0] = widen(inv[0])
    solve(0, 0, 0, True)
    pl.semaphore_wait(barrier, targets + jnp.where(leads, followers, 0))

    send_direct(0)
    second.wait()
    for load in maps + loads:
        load.start()

    def first_level(w, carry):
        solve(w, 0, w, True)
        send_direct(w)
        return carry

    lax.fori_loop(1, chunks, first_level, 0)
    gather_plane()
    for load in maps:
        load.wait()
    lax.fori_loop(0, depth, tables, 0)
    chain[0] = jnp.zeros(chain.shape[1:], jnp.float32)

    def clear(n, carry):
        pending[n // codes, lax.rem(n, codes)] = jnp.zeros(pending.shape[2:], jnp.float32)
        return carry

    lax.fori_loop(0, chunks * codes, clear, 0)
    for load in loads:
        load.wait()
    for k in range(1, depth):
        wide[k] = widen(inv[k])
    wide[depth] = widen(anc_inv[...])

    def middle(i, carry):
        spread(i, i // chunks, lax.rem(i, chunks))

        @pl.when(i + 1 < steps)
        def _():
            relays(i + 1, pass_on)
            release(i + 1)

        later = i + chunks - LAG

        @pl.when((i >= LAG) & (later < steps))
        def _():
            solve(later, later // chunks, lax.rem(later, chunks), False)
            send_direct(later)

        @pl.when(later >= steps + 1)
        def _():
            finish(later - steps - 1)

        pl.when(later >= steps + 3)(lambda: deliver(later - steps - 3))
        pl.when(i >= BEHIND)(lambda: drain(i - BEHIND))
        return carry

    def deliver(w):
        owner = lax.rem(w, n_grp)

        @pl.when(owner != g)
        def _():
            anc_copy(w, g).wait_recv()

        anc_out[:, cols(w)] = anc_box[w]

        @pl.when(owner == g)
        def _():
            for e in range(1, n_grp):
                anc_copy(w, lax.rem(g + e, n_grp)).wait_send()

    def drain(i):
        each_direct(i, lambda copy, wait_turn: copy.wait_send())
        relays(i, lambda arrived, onward: onward.wait_send())
        to_g = jnp.where(i < (depth - 1) * chunks, g, lax.rem(lax.rem(i, chunks), n_grp))
        for d in range(1, n_row):
            rs_copy(i, g, q, to_g, lax.rem(q + d, n_row)).wait_send()

        @pl.when(to_g != g)
        def _():
            rs_copy(i, g, q, to_g, q).wait_send()

    await_plane()
    relays(0, pass_on)
    release(0)
    lax.fori_loop(0, steps, middle, 0)
    for w in range(max(chunks - LAG - 1, 0), chunks):
        finish(jnp.int32(w))
    for i in range(steps - BEHIND, steps):
        drain(jnp.int32(i))
    for w in range(max(chunks - LAG - 3, 0), chunks):
        deliver(jnp.int32(w))


def hand_over(sub_ref, anc_ref, sub_out, anc_out, sem):
    copies = [
        pltpu.make_async_copy(sub_ref, sub_out, sem.at[0]),
        pltpu.make_async_copy(anc_ref, anc_out, sem.at[1]),
    ]
    for copy in copies:
        copy.start()
    for copy in copies:
        copy.wait()


def on_device(mesh, sub_rhs, sub_dinv, anc_rhs, anc_dinv, tiles, tile_target, tile_source, tile_count):
    n_grp, n_row, n_col = mesh.shape["grp"], mesh.shape["row"], mesh.shape["col"]
    depth, size, width = sub_rhs.shape[1], sub_rhs.shape[4], sub_rhs.shape[5]
    slots = tiles.shape[4]
    chunks = width // CHUNK
    steps = depth * chunks
    codes = depth * n_row
    bf16, f32 = jnp.bfloat16, jnp.float32
    dma = pltpu.SemaphoreType.DMA
    sub, anc = pl.pallas_call(
        functools.partial(kernel, n_grp, n_row, n_col),
        out_shape=(
            pltpu.VMEM((depth, size, width), f32),
            pltpu.VMEM((size, width), f32),
        ),
        in_specs=[pl.BlockSpec(memory_space=pltpu.HBM)] * 8,
        out_specs=(pl.BlockSpec(memory_space=pltpu.VMEM), pl.BlockSpec(memory_space=pltpu.VMEM)),
        scratch_shapes=[
            pltpu.VMEM((depth, size, width), f32),
            pltpu.VMEM((depth, size, size), f32),
            pltpu.VMEM((size, width), f32),
            pltpu.VMEM((size, size), f32),
            pltpu.VMEM((depth, slots, size, size), bf16),
            pltpu.VMEM((depth + 1, size, 3 * size), bf16),
            pltpu.VMEM((steps, n_col, size, CHUNK), bf16),
            pltpu.VMEM((n_col, size, CHUNK), bf16),
            pltpu.VMEM((slots + 1, size, CHUNK), f32),
            pltpu.VMEM((chunks, codes, size, CHUNK), f32),
            pltpu.VMEM((steps, n_row, size, CHUNK), bf16),
            pltpu.VMEM((steps, n_grp * n_row, size, CHUNK), bf16),
            pltpu.VMEM((chunks, size, CHUNK), f32),
            pltpu.SMEM((depth, 1, slots), jnp.int32),
            pltpu.SMEM((depth, 1, slots), jnp.int32),
            pltpu.SMEM((1, 1, 1, depth), jnp.int32),
            pltpu.SMEM((depth * slots,), jnp.int32),
            pltpu.SMEM((depth * codes,), jnp.int32),
            pltpu.SMEM((depth * slots,), jnp.int32),
            dma((11,)),
            dma((steps, n_col)),
            dma((steps, n_col)),
            dma((steps, max(len(hops(n_col)), 1))),
            dma((steps, n_row)),
            dma((steps, n_grp * n_row)),
            dma((chunks, n_grp)),
            dma((chunks,)),
            pltpu.SemaphoreType.REGULAR,
        ],
        compiler_params=pltpu.CompilerParams(
            collective_id=0, has_side_effects=True, vmem_limit_bytes=67_043_328 - 4 * (depth + 1) * size * width
        ),
    )(
        tile_target.reshape(depth, 1, slots), tile_source.reshape(depth, 1, slots), tile_count,
        sub_rhs.reshape(depth, size, width), sub_dinv.reshape(depth, size, size),
        anc_rhs.reshape(size, width), anc_dinv.reshape(size, size),
        tiles.reshape(depth, slots, size, size),
    )
    sub, anc = pl.pallas_call(
        hand_over,
        out_shape=(
            jax.ShapeDtypeStruct((depth, size, width), f32),
            jax.ShapeDtypeStruct((size, width), f32),
        ),
        in_specs=[pl.BlockSpec(memory_space=pl.ANY)] * 2,
        out_specs=(pl.BlockSpec(memory_space=pl.ANY), pl.BlockSpec(memory_space=pl.ANY)),
        scratch_shapes=[dma((2,))],
        compiler_params=pltpu.CompilerParams(vmem_limit_bytes=1 << 20),
    )(sub, anc)
    return sub[None, :, None, None], anc[None, None]


def solution(mesh):
    placed = (
        P("grp", None, "row", "col", None, None),
        P("grp", None, "row", "col", None, None),
        P("row", "col", None, None),
        P("row", "col", None, None),
        P("grp", "row", "col", None, None, None, None),
        P("grp", "row", "col", None, None),
        P("grp", "row", "col", None, None),
        P("grp", "row", "col", None),
    )
    return jax.shard_map(
        functools.partial(on_device, mesh),
        mesh=mesh,
        in_specs=placed,
        out_specs=(P("grp", None, "row", "col", None, None), P("row", "col", None, None)),
        check_vma=False,
    )
```

```python
import functools

import jax
import jax.numpy as jnp
from jax import lax
from jax.experimental import pallas as pl
from jax.experimental.pallas import tpu as pltpu
from jax.sharding import PartitionSpec as P

MESH = pl.DeviceIdType.MESH
CHUNK = 128
AHEAD = 3
LAG = 1
BEHIND = 3


def hops(n_col):
    if not 2 < n_col <= 4:
        return ()
    up = [(o, n_col - 2, n_col - 1) for o in reversed(range(n_col - 2))]
    down = [(o, 1, 0) for o in range(2, n_col)]
    return tuple(up + down)


def kernel(
    n_grp, n_row, n_col,
    target_hbm, source_hbm, count_hbm,
    rhs_hbm, inv_hbm, anc_rhs_hbm, anc_inv_hbm, tiles_hbm,
    sub_out, anc_out,
    rhs, inv, anc_rhs, anc_inv, tiles, wide,
    gathered, fetched, chain, pending, outbox, inbox, anc_box,
    target_ref, source_ref, count_ref, prev_s, last_s, src_s,
    load_sem, ag_send, ag_recv, fwd_send, rs_send, rs_recv, anc_send, anc_recv, plane_sem,
):
    depth, size, width = rhs.shape
    slots = tiles.shape[1]
    chunks = width // CHUNK
    steps = depth * chunks
    codes = depth * n_row
    passes = hops(n_col)
    g = lax.axis_index("grp")
    q = lax.axis_index("row")
    c = lax.axis_index("col")

    early = [
        pltpu.make_async_copy(inv_hbm.at[0], inv.at[0], load_sem.at[0]),
        pltpu.make_async_copy(rhs_hbm.at[0, :, pl.ds(0, CHUNK)], rhs.at[0, :, pl.ds(0, CHUNK)], load_sem.at[1]),
    ]
    others = pl.ds(CHUNK, width - CHUNK)
    second = pltpu.make_async_copy(rhs_hbm.at[0, :, others], rhs.at[0, :, others], load_sem.at[10])
    maps = [
        pltpu.make_async_copy(target_hbm, target_ref, load_sem.at[7]),
        pltpu.make_async_copy(source_hbm, source_ref, load_sem.at[8]),
        pltpu.make_async_copy(count_hbm, count_ref, load_sem.at[9]),
    ]
    loads = [
        pltpu.make_async_copy(tiles_hbm, tiles, load_sem.at[2]),
        pltpu.make_async_copy(anc_rhs_hbm, anc_rhs, load_sem.at[3]),
        pltpu.make_async_copy(anc_inv_hbm, anc_inv, load_sem.at[4]),
    ]
    if depth > 1:
        loads += [
            pltpu.make_async_copy(inv_hbm.at[pl.ds(1, depth - 1)], inv.at[pl.ds(1, depth - 1)], load_sem.at[5]),
            pltpu.make_async_copy(rhs_hbm.at[pl.ds(1, depth - 1)], rhs.at[pl.ds(1, depth - 1)], load_sem.at[6]),
        ]
    for load in early + [second]:
        load.start()

    barrier = pltpu.get_barrier_semaphore()
    targets = n_col - 1
    for owner, relay, end in passes:
        targets = targets - (c == owner).astype(jnp.int32)
    for d in range(1, n_col):
        peer = lax.rem(c + d, n_col)
        writes_here = True
        for owner, relay, end in passes:
            writes_here = writes_here & jnp.logical_not((peer == owner) & (c == end))

        @pl.when(writes_here)
        def _():
            pl.semaphore_signal(barrier, inc=1, device_id=(g, q, peer), device_id_type=MESH)

    leads = (g == 0) & (q == n_row - 1)
    followers = n_grp * n_row - 1

    @pl.when(jnp.logical_not(leads))
    def _():
        pl.semaphore_signal(barrier, inc=1, device_id=(0, n_row - 1, c), device_id_type=MESH)

    def gather_plane():
        @pl.when(leads)
        def _():
            for e in range(n_grp):
                for d in range(n_row):
                    if e or d:
                        pl.semaphore_signal(
                            plane_sem, inc=1,
                            device_id=(lax.rem(g + e, n_grp), lax.rem(q + d, n_row), c), device_id_type=MESH,
                        )

    def await_plane():
        @pl.when(jnp.logical_not(leads))
        def _():
            pl.semaphore_wait(plane_sem, 1)

    def tables(k, carry):
        count = count_ref[0, 0, 0, k]
        raw = [target_ref[k, 0, j] for j in range(slots)]
        live = [jnp.where(j < count, raw[j], -1) for j in range(slots)]
        for j in range(slots):
            found = jnp.int32(0)
            for i in range(j):
                found = jnp.where(raw[i] == raw[j], i + 1, found)
            prev_s[k * slots + j] = found
            src_s[k * slots + j] = jnp.clip(source_ref[k, 0, j], 0, n_col - 1)
        for code in range(codes):
            found = jnp.int32(0)
            for j in range(slots):
                found = jnp.where(live[j] == code, j + 1, found)
            last_s[k * codes + code] = found
        return carry

    def cols(w):
        return pl.ds(pl.multiple_of(w * CHUNK, CHUNK), CHUNK)

    def ag_copy(i, owner, peer):
        return pltpu.make_async_remote_copy(
            src_ref=gathered.at[i, owner], dst_ref=gathered.at[i, owner],
            send_sem=ag_send.at[i, peer], recv_sem=ag_recv.at[i, owner],
            device_id=(g, q, peer), device_id_type=MESH,
        )

    def relays(i, run):
        for way, (owner, relay, end) in enumerate(passes):

            @pl.when(c == relay)
            def _():
                run(
                    ag_copy(i, owner, c),
                    pltpu.make_async_remote_copy(
                        src_ref=gathered.at[i, owner], dst_ref=gathered.at[i, owner],
                        send_sem=fwd_send.at[i, way], recv_sem=ag_recv.at[i, owner],
                        device_id=(g, q, end), device_id_type=MESH,
                    ),
                )

    def each_direct(i, run):
        for d in range(1, n_col):
            peer = lax.rem(c + d, n_col)
            far = False
            for owner, relay, end in passes:
                far = far | ((c == owner) & (peer == end))

            @pl.when(jnp.logical_not(far))
            def _():
                run(ag_copy(i, c, peer), held(i, peer))

    def held(i, peer):
        if not passes:
            return False
        to_end = ((c == n_col - 2) & (peer == n_col - 1)) | ((c == 1) & (peer == 0))
        return to_end & (i >= AHEAD) & (i < chunks)

    def send_direct(i):
        def start(copy, wait_turn):
            pl.when(jnp.logical_not(wait_turn))(copy.start)

        each_direct(i, start)

    def release(i):
        for relay, end in ((n_col - 2, n_col - 1), (1, 0)):
            if passes:

                @pl.when((c == relay) & (i + AHEAD < chunks))
                def _():
                    ag_copy(i + AHEAD, c, end).start()

    def rs_copy(i, owner_g, owner_q, to_g, to_q):
        return pltpu.make_async_remote_copy(
            src_ref=outbox.at[i, to_q], dst_ref=inbox.at[i, owner_g * n_row + owner_q],
            send_sem=rs_send.at[i, to_q], recv_sem=rs_recv.at[i, owner_g * n_row + owner_q],
            device_id=(to_g, to_q, c), device_id_type=MESH,
        )

    def anc_copy(w, peer_g):
        return pltpu.make_async_remote_copy(
            src_ref=anc_box.at[w], dst_ref=anc_box.at[w],
            send_sem=anc_send.at[w, peer_g], recv_sem=anc_recv.at[w],
            device_id=(peer_g, q, c), device_id_type=MESH,
        )

    def full_dot(a, b):
        high = b.astype(jnp.bfloat16)
        low = (b - high.astype(jnp.float32)).astype(jnp.bfloat16)
        return jnp.dot(a, jnp.concatenate([high, low, high], axis=0), preferred_element_type=jnp.float32)

    def widen(a):
        high = a.astype(jnp.bfloat16)
        low = (a - high.astype(jnp.float32)).astype(jnp.bfloat16)
        return jnp.concatenate([high, high, low], axis=1)

    def solve(i, k, w, first):
        rest = rhs[k, :, cols(w)]
        if not first:
            back = i - chunks
            total = pending[w, (k - 1) * n_row + q]
            for d in range(1, n_row):
                other = lax.rem(q + d, n_row)
                rs_copy(back, g, other, g, q).wait_recv()
                total = total + inbox[back, g * n_row + other].astype(jnp.float32)
            rest = rest - total
        answer = full_dot(wide[k], rest)
        sub_out[k, :, cols(w)] = answer
        gathered[i, c] = answer.astype(jnp.bfloat16)

    def pass_on(arrived, onward):
        arrived.wait_recv()
        onward.start()

    def spread(i, k, w):
        fetched[c] = gathered[i, c]
        for d in range(1, n_col):
            other = lax.rem(c + jnp.where(c < n_col // 2, d, n_col - d), n_col)
            passed = False
            for owner, relay, end in passes:
                passed = passed | ((c == relay) & (other == owner))

            @pl.when(jnp.logical_not(passed))
            def _():
                ag_copy(i, other, c).wait_recv()

            fetched[other] = gathered[i, other]

        for j in range(slots):
            product = jnp.dot(
                tiles[k, j], fetched[src_s[k * slots + j]], preferred_element_type=jnp.float32
            )
            chain[j + 1] = product + chain[prev_s[k * slots + j]]

        def updated(code):
            return pending[w, code] + chain[last_s[k * codes + code]]

        to_g = jnp.where(k < depth - 1, g, lax.rem(w, n_grp))
        for d in list(range(1, n_row)) + [0]:
            to_q = lax.rem(q + d, n_row)
            value = updated(k * n_row + to_q)

            def send():
                outbox[i, to_q] = value.astype(jnp.bfloat16)
                rs_copy(i, g, q, to_g, to_q).start()

            if d == 0:
                pending[w, k * n_row + q] = value
                pl.when(to_g != g)(send)
            else:
                send()

        def collect(code, carry):
            pending[w, code] = updated(code)
            return carry

        lax.fori_loop((k + 1) * n_row, codes, collect, 0)

    def finish(w):
        i = (depth - 1) * chunks + w

        @pl.when(lax.rem(w, n_grp) == g)
        def _():
            total = pending[w, (depth - 1) * n_row + q]
            for e in range(n_grp):
                for d in range(n_row):
                    if e or d:
                        other_g, other_q = lax.rem(g + e, n_grp), lax.rem(q + d, n_row)
                        rs_copy(i, other_g, other_q, g, q).wait_recv()
                        total = total + inbox[i, other_g * n_row + other_q].astype(jnp.float32)
            anc_box[w] = full_dot(wide[depth], anc_rhs[:, cols(w)] - total)
            for e in range(1, n_grp):
                anc_copy(w, lax.rem(g + e, n_grp)).start()

    for load in early:
        load.wait()
    wide[0] = widen(inv[0])
    solve(0, 0, 0, True)
    pl.semaphore_wait(barrier, targets + jnp.where(leads, followers, 0))

    send_direct(0)
    second.wait()
    for load in maps + loads:
        load.start()

    def first_level(w, carry):
        solve(w, 0, w, True)
        send_direct(w)
        return carry

    lax.fori_loop(1, chunks, first_level, 0)
    gather_plane()
    for load in maps:
        load.wait()
    lax.fori_loop(0, depth, tables, 0)
    chain[0] = jnp.zeros(chain.shape[1:], jnp.float32)

    def clear(n, carry):
        pending[n // codes, lax.rem(n, codes)] = jnp.zeros(pending.shape[2:], jnp.float32)
        return carry

    lax.fori_loop(0, chunks * codes, clear, 0)
    for load in loads:
        load.wait()
    for k in range(1, depth):
        wide[k] = widen(inv[k])
    wide[depth] = widen(anc_inv[...])

    def middle(i, carry):
        spread(i, i // chunks, lax.rem(i, chunks))

        @pl.when(i + 1 < steps)
        def _():
            relays(i + 1, pass_on)
            release(i + 1)

        later = i + chunks - LAG

        @pl.when((i >= LAG) & (later < steps))
        def _():
            solve(later, later // chunks, lax.rem(later, chunks), False)
            send_direct(later)

        pl.when(i >= BEHIND)(lambda: drain(i - BEHIND))
        return carry

    def deliver(w):
        owner = lax.rem(w, n_grp)

        @pl.when(owner != g)
        def _():
            anc_copy(w, g).wait_recv()

        anc_out[:, cols(w)] = anc_box[w]

        @pl.when(owner == g)
        def _():
            for e in range(1, n_grp):
                anc_copy(w, lax.rem(g + e, n_grp)).wait_send()

    def drain(i):
        each_direct(i, lambda copy, wait_turn: copy.wait_send())
        relays(i, lambda arrived, onward: onward.wait_send())
        to_g = jnp.where(i < (depth - 1) * chunks, g, lax.rem(lax.rem(i, chunks), n_grp))
        for d in range(1, n_row):
            rs_copy(i, g, q, to_g, lax.rem(q + d, n_row)).wait_send()

        @pl.when(to_g != g)
        def _():
            rs_copy(i, g, q, to_g, q).wait_send()

    await_plane()
    relays(0, pass_on)
    release(0)
    lax.fori_loop(0, steps, middle, 0)
    for w in range(chunks):
        finish(jnp.int32(w))
    for i in range(steps - BEHIND, steps):
        drain(jnp.int32(i))
    for w in range(chunks):
        deliver(jnp.int32(w))


def hand_over(sub_ref, anc_ref, sub_out, anc_out, sem):
    copies = [
        pltpu.make_async_copy(sub_ref, sub_out, sem.at[0]),
        pltpu.make_async_copy(anc_ref, anc_out, sem.at[1]),
    ]
    for copy in copies:
        copy.start()
    for copy in copies:
        copy.wait()


def on_device(mesh, sub_rhs, sub_dinv, anc_rhs, anc_dinv, tiles, tile_target, tile_source, tile_count):
    n_grp, n_row, n_col = mesh.shape["grp"], mesh.shape["row"], mesh.shape["col"]
    depth, size, width = sub_rhs.shape[1], sub_rhs.shape[4], sub_rhs.shape[5]
    slots = tiles.shape[4]
    chunks = width // CHUNK
    steps = depth * chunks
    codes = depth * n_row
    bf16, f32 = jnp.bfloat16, jnp.float32
    dma = pltpu.SemaphoreType.DMA
    sub, anc = pl.pallas_call(
        functools.partial(kernel, n_grp, n_row, n_col),
        out_shape=(
            pltpu.VMEM((depth, size, width), f32),
            pltpu.VMEM((size, width), f32),
        ),
        in_specs=[pl.BlockSpec(memory_space=pltpu.HBM)] * 8,
        out_specs=(pl.BlockSpec(memory_space=pltpu.VMEM), pl.BlockSpec(memory_space=pltpu.VMEM)),
        scratch_shapes=[
            pltpu.VMEM((depth, size, width), f32),
            pltpu.VMEM((depth, size, size), f32),
            pltpu.VMEM((size, width), f32),
            pltpu.VMEM((size, size), f32),
            pltpu.VMEM((depth, slots, size, size), bf16),
            pltpu.VMEM((depth + 1, size, 3 * size), bf16),
            pltpu.VMEM((steps, n_col, size, CHUNK), bf16),
            pltpu.VMEM((n_col, size, CHUNK), bf16),
            pltpu.VMEM((slots + 1, size, CHUNK), f32),
            pltpu.VMEM((chunks, codes, size, CHUNK), f32),
            pltpu.VMEM((steps, n_row, size, CHUNK), bf16),
            pltpu.VMEM((steps, n_grp * n_row, size, CHUNK), bf16),
            pltpu.VMEM((chunks, size, CHUNK), f32),
            pltpu.SMEM((depth, 1, slots), jnp.int32),
            pltpu.SMEM((depth, 1, slots), jnp.int32),
            pltpu.SMEM((1, 1, 1, depth), jnp.int32),
            pltpu.SMEM((depth * slots,), jnp.int32),
            pltpu.SMEM((depth * codes,), jnp.int32),
            pltpu.SMEM((depth * slots,), jnp.int32),
            dma((11,)),
            dma((steps, n_col)),
            dma((steps, n_col)),
            dma((steps, max(len(hops(n_col)), 1))),
            dma((steps, n_row)),
            dma((steps, n_grp * n_row)),
            dma((chunks, n_grp)),
            dma((chunks,)),
            pltpu.SemaphoreType.REGULAR,
        ],
        compiler_params=pltpu.CompilerParams(
            collective_id=0, has_side_effects=True, vmem_limit_bytes=67_043_328 - 4 * (depth + 1) * size * width
        ),
    )(
        tile_target.reshape(depth, 1, slots), tile_source.reshape(depth, 1, slots), tile_count,
        sub_rhs.reshape(depth, size, width), sub_dinv.reshape(depth, size, size),
        anc_rhs.reshape(size, width), anc_dinv.reshape(size, size),
        tiles.reshape(depth, slots, size, size),
    )
    sub, anc = pl.pallas_call(
        hand_over,
        out_shape=(
            jax.ShapeDtypeStruct((depth, size, width), f32),
            jax.ShapeDtypeStruct((size, width), f32),
        ),
        in_specs=[pl.BlockSpec(memory_space=pl.ANY)] * 2,
        out_specs=(pl.BlockSpec(memory_space=pl.ANY), pl.BlockSpec(memory_space=pl.ANY)),
        scratch_shapes=[dma((2,))],
        compiler_params=pltpu.CompilerParams(vmem_limit_bytes=1 << 20),
    )(sub, anc)
    return sub[None, :, None, None], anc[None, None]


def solution(mesh):
    placed = (
        P("grp", None, "row", "col", None, None),
        P("grp", None, "row", "col", None, None),
        P("row", "col", None, None),
        P("row", "col", None, None),
        P("grp", "row", "col", None, None, None, None),
        P("grp", "row", "col", None, None),
        P("grp", "row", "col", None, None),
        P("grp", "row", "col", None),
    )
    return jax.shard_map(
        functools.partial(on_device, mesh),
        mesh=mesh,
        in_specs=placed,
        out_specs=(P("grp", None, "row", "col", None, None), P("row", "col", None, None)),
        check_vma=False,
    )
```
